32 devices in a mesh: cfd: 16 (over z, x, core), ac: 2 (over y).
Axes of the slice: x: 2, y: 2, z: 4, core: 2. Of those that a mesh axis runs over, the one named last changes fastest.
Arguments:
- surface_raw: bfloat16 [5, 4096, 1024], P(None, ('cfd', 'ac')), may hold values from -6 to 6
- area_normals: bfloat16 [3, 4096], P(None, ('cfd', 'ac')), may hold values from -6 to 6
- kernel_weights: bfloat16 [2, 3, 2048, 4096], P(None, None, None, ('cfd', 'ac')), may hold values from -0.078125 to 0.078125
- block_map: int32 [2, 16, 16], P('ac', 'cfd'), may hold values from 0 to 15, as said below
- band_observers: int32 [16, 128], replicated, may hold values from 0 to 2047, as said below
- band_lags: int32 [16], replicated, may hold values from 0 to 511
Outputs:
- acoustic: float32 [2048, 512], P('cfd', 'ac')
The draws below stay inside these ranges and needn't reach their ends.
Inputs may be any that keep to these rules, and one draw needn't show every extreme that they name: block_map[j, s, :] is a permutation of 0 to 15 for every j and s. `band_observers`: every observer appears exactly once.
All inputs are finite; a program needn't handle non-finite values.
Results may differ from the reference program's by a relative error of at most 0.0042.
Values may be sent and summed in bfloat16 or wider, within the bound.
No kernel may reach another device: no remote copies, remote signals or barrier semaphores. Data moves between devices by JAX's collectives and lax.ppermute only.
A program may use at most 64 MiB of HBM per device.

```python
import jax
import jax.numpy as jnp
from jax import lax

OBS = 2048
BANDS = 16
OBS_BAND = 128
TAPS = 2
BLOCK = 8
FACES = 4096
WINDOW = 1024
OUT_STEPS = 512
N_CFD = 16
N_AC = 2


def draw_band_observers(key, part):
    shuffled = jax.random.permutation(jax.random.fold_in(key, 11), OBS)
    return shuffled.astype(jnp.int32).reshape(BANDS, OBS // BANDS)


def draw_block_map(key, part):
    key_list = jax.random.split(jax.random.fold_in(key, 23), N_AC * N_CFD)
    orders = jax.vmap(lambda single_key: jax.random.permutation(single_key, N_CFD))(key_list)
    return orders.astype(jnp.int32).reshape(N_AC, N_CFD, N_CFD)


def set_ends(entries, stream_key, low, top_value):
    longest = entries.shape.index(max(entries.shape))
    spots = []
    for shift in (0, 1):
        where = [jax.random.randint(jax.random.fold_in(stream_key, axis), (), 0, length) for axis, length in enumerate(entries.shape)]
        where[longest] = (where[longest] + shift) % entries.shape[longest]
        spots.append(tuple(where))
    return entries.at[spots[0]].set(low).at[spots[1]].set(top_value)


def spiked(entries, rng, source, target, parts, factor):
    owner, partner = [(jnp.arange(entries.shape[axis_at]) // (entries.shape[axis_at] // parts)).reshape([-1 if axis == axis_at else 1 for axis in range(entries.ndim)]) for axis_at in (source, target)]
    chosen = jax.random.permutation(rng, parts)[partner]
    strong = (owner == chosen) | (owner == (partner + parts // 2) % parts)
    return jnp.where(strong, factor * entries, entries)


def block_scale(rng, shape, pieces, least, high):
    def one(dim, shards_of):
        draws = jax.random.uniform(jax.random.fold_in(jax.random.fold_in(rng, 6), dim), (shards_of,), jnp.float32, least / len(pieces), high / len(pieces))
        return jnp.repeat(jnp.exp(draws), shape[dim] // shards_of).reshape((-1,) + (1,) * (len(shape) - dim - 1))

    factor_of = one(*pieces[0])
    for cut in pieces[1:]:
        factor_of = factor_of * one(*cut)
    return factor_of


def gaussian(rng, dims, width, most, cuts=(), kind=jnp.bfloat16):
    values = width * jax.random.normal(rng, dims, jnp.float32)
    if cuts:
        values = values * block_scale(rng, dims, cuts, -0.22, 0.18)
    return jnp.clip(values, -most, most).astype(kind)


def gaussian_with(key, dims, scale, limit, cuts, heavy, held_as=jnp.bfloat16):
    result = scale * jax.random.normal(key, dims, jnp.float32)
    if cuts:
        result = result * block_scale(key, dims, cuts, -0.22, 0.18)
    return jnp.clip(spiked(result, jax.random.fold_in(key, 3), *heavy), -limit, limit).astype(held_as)


def setup_inputs(seed: int = 0) -> dict:
    seeds = jax.random.split(jax.random.key(seed), 7)
    surface_raw = gaussian(seeds[0], (5, FACES, WINDOW), 1.0, 6.0, ((1, 32),))
    area_normals = gaussian(seeds[1], (3, FACES), 1.0, 6.0, ((1, 32),))
    kernel_weights = gaussian_with(seeds[2], (TAPS, 3, OBS, FACES), (6 * FACES) ** -0.5, 0.078125, ((3, 32),), (3, 2, 32, 2.75))
    block_map = draw_block_map(jax.random.fold_in(seeds[6], 71), 0)
    band_observers = draw_band_observers(jax.random.fold_in(seeds[6], 71), 0)
    band_lags = set_ends(jax.random.randint(seeds[5], (BANDS,), 0, OUT_STEPS), jax.random.fold_in(seeds[5], 1), 0, OUT_STEPS - 1).astype(jnp.int32)
    return dict(surface_raw=surface_raw, area_normals=area_normals, kernel_weights=kernel_weights, block_map=block_map, band_observers=band_observers, band_lags=band_lags)


def thickness(surface, normals):
    along = surface[2].astype(jnp.float32) * normals[0].astype(jnp.float32)[:, None]
    along = along + surface[3].astype(jnp.float32) * normals[1].astype(jnp.float32)[:, None]
    along = along + surface[4].astype(jnp.float32) * normals[2].astype(jnp.float32)[:, None]
    return (surface[1].astype(jnp.float32) * along).astype(jnp.bfloat16)


def rates(series):
    step = series[:, 1:].astype(jnp.float32) - series[:, :-1].astype(jnp.float32)
    first = jnp.zeros((series.shape[0], 1), jnp.float32)
    return jnp.concatenate([first, step], axis=1).astype(jnp.bfloat16)


def reference(surface_raw, area_normals, kernel_weights, block_map, band_observers, band_lags):
    thick = thickness(surface_raw, area_normals)
    stacked = jnp.stack([thick, surface_raw[0]])
    shaped = stacked.reshape(2, N_CFD, N_AC, N_CFD, BLOCK, WINDOW)
    picks = jnp.transpose(block_map, (1, 0, 2))[None, :, :, :, None, None]
    moved = jnp.take_along_axis(shaped, picks, axis=3)
    moved = jnp.transpose(moved, (0, 3, 2, 1, 4, 5)).reshape(2, FACES, WINDOW)
    sources = jnp.stack([rates(moved[0]), rates(moved[1]), moved[1]])

    def one_band(acoustic, band_index):
        members = band_observers[band_index]
        delay = band_lags[band_index]
        start = (band_index * OBS_BAND).astype(jnp.int32)
        chosen = lax.dynamic_slice_in_dim(kernel_weights, start, OBS_BAND, 2).astype(jnp.float32)
        windows = jnp.stack([lax.dynamic_slice_in_dim(sources, (OUT_STEPS - delay - shift_step).astype(jnp.int32), OUT_STEPS, 2) for shift_step in range(TAPS)]).astype(jnp.float32)
        contribution = jnp.einsum("kcof,kcft->ot", chosen, windows, precision=lax.Precision.HIGHEST)
        return acoustic.at[members].set(contribution), None

    initial = jnp.zeros((OBS, OUT_STEPS), jnp.float32)
    acoustic, _ = lax.scan(one_band, initial, jnp.arange(BANDS, dtype=jnp.int32))
    return acoustic
```

```python
import functools

import jax
import jax.numpy as jnp
from jax import lax
from jax.experimental import pallas as pl
from jax.experimental.pallas import tpu as pltpu
from jax.sharding import PartitionSpec as P

LANES = 128
AXES = ("cfd", "ac")
SMEM = pl.BlockSpec(memory_space=pltpu.SMEM)
VMEM = pl.BlockSpec(memory_space=pltpu.VMEM)


def outgoing_kernel(blocks, order_ref, surface_ref, normals_ref, out_ref):
    normals = normals_ref[...].astype(jnp.float32)
    rows = surface_ref.shape[2]
    faces = normals.shape[1]
    square = jnp.concatenate([normals, jnp.zeros((faces - normals.shape[0], faces), jnp.float32)], axis=0)
    columns = jnp.transpose(square)
    picked = [columns[p * rows : (p + 1) * rows, :] for p in range(blocks)]
    for p in range(blocks):
        along = surface_ref[2, p].astype(jnp.float32) * picked[p][:, 0:1]
        along = along + surface_ref[3, p].astype(jnp.float32) * picked[p][:, 1:2]
        along = along + surface_ref[4, p].astype(jnp.float32) * picked[p][:, 2:3]
        to = order_ref[p]
        out_ref[to, 0] = (surface_ref[1, p].astype(jnp.float32) * along).astype(jnp.bfloat16)
        out_ref[to, 1] = surface_ref[0, p]


def outgoing(surface, normals, block_to):
    blocks = block_to.shape[0]
    comps, faces, steps = surface.shape
    rows = faces // blocks
    return pl.pallas_call(
        functools.partial(outgoing_kernel, blocks),
        out_shape=jax.ShapeDtypeStruct((blocks, 2, rows, steps), jnp.bfloat16),
        in_specs=[SMEM, VMEM, VMEM],
        out_specs=VMEM,
        name="outgoing",
    )(block_to, surface.reshape(comps, blocks, rows, steps), normals)


def bands_kernel(
    split, cols, me_ref, lags_ref, observers_ref, arrived_ref, weights_ref, keep_ref, send_ref,
    stacked_ref, banded_ref, select_ref,
):
    taps, terms, observers, faces = weights_ref.shape
    blocks, _, rows, steps = arrived_ref.shape
    span = stacked_ref.shape[1]
    out_len = banded_ref.shape[1]
    bands = lags_ref.shape[0]
    width = observers // bands
    wide = out_len + LANES
    pad = jnp.zeros((faces, span - steps), jnp.bfloat16)
    for kind in range(2):
        series = jnp.concatenate([arrived_ref[s, kind].astype(jnp.float32) for s in range(blocks)], axis=0)
        earlier = pltpu.roll(series, 1, 1)
        first = lax.broadcasted_iota(jnp.int32, series.shape, 1) == 0
        rate = jnp.where(first, 0.0, series - earlier)
        made = [(kind, rate)] if kind == 0 else [(1, rate), (2, series)]
        for term, value in made:
            for tap in range(taps):
                moved = pltpu.roll(value, tap, 1) if tap else value
                at = (tap * terms + term) * faces
                stacked_ref[at : at + faces, 0:steps] = moved.astype(jnp.bfloat16)
                stacked_ref[at : at + faces, steps:span] = pad

    def one_band(b, carry):
        start = out_len - lags_ref[b]
        column = pl.multiple_of((start // LANES) * LANES, LANES)
        rest = start % LANES
        at = pl.ds(pl.multiple_of(b * width, width), width)
        chosen = jnp.concatenate(
            [weights_ref[k, c, at, :] for k in range(taps) for c in range(terms)], axis=1
        )
        full = jnp.dot(chosen, stacked_ref[:, pl.ds(column, wide)], preferred_element_type=jnp.float32)
        turned = pltpu.roll(full, (wide - rest) % wide, 1)
        banded_ref[at, :] = turned[:, :out_len].astype(jnp.bfloat16)
        return carry

    lax.fori_loop(0, bands, one_band, 0)

    ranks, sides, parts = split
    each = observers // ranks
    ids = observers_ref[...]
    low = 2 if ranks % 2 == 0 else 1
    mid = 2 if ranks % 4 == 0 else 1
    rest_count = ranks // low // mid
    for c in range(low):
        out_ref = keep_ref if c == 0 else send_ref
        for x in range(mid):
            for z in range(rest_count):
                member = (z * mid + x) * low + c
                base = jnp.bitwise_xor(me_ref[0], member) * each
                row = lax.broadcasted_iota(jnp.int32, (each, observers), 0) + base
                select_ref[z * each : (z + 1) * each, :] = jnp.where(row == ids, 1.0, 0.0).astype(jnp.bfloat16)
            for y in range(parts):
                if parts == 1:
                    data = banded_ref[...]
                else:
                    piece = out_len // parts
                    at = pl.multiple_of(jnp.bitwise_xor(me_ref[1], y) * piece, piece)
                    data = banded_ref[:, pl.ds(at, piece)]
                picked = jnp.dot(select_ref[...], data, preferred_element_type=jnp.float32)
                picked = picked.astype(jnp.bfloat16)
                for z in range(rest_count):
                    out_ref[x, y, z] = picked[z * each : (z + 1) * each, :]


def bands(me, lags, observers, arrived, weights, ranks, sides):
    taps, terms, count, faces = weights.shape
    steps = arrived.shape[3]
    out_len = steps // 2
    piece = out_len // sides
    parts = sides if piece % LANES == 0 else 1
    low = 2 if ranks % 2 == 0 else 1
    mid = 2 if ranks % 4 == 0 else 1
    rest = ranks // low // mid
    each = count // ranks
    shape = jax.ShapeDtypeStruct((mid, parts, rest, each, out_len // parts), jnp.bfloat16)
    return pl.pallas_call(
        functools.partial(bands_kernel, (ranks, sides, parts), out_len),
        out_shape=(shape, shape),
        in_specs=[SMEM, SMEM, VMEM, VMEM, VMEM],
        out_specs=(VMEM, VMEM),
        scratch_shapes=[
            pltpu.VMEM((taps * terms * faces, steps + LANES), jnp.bfloat16),
            pltpu.VMEM((count, out_len), jnp.bfloat16),
            pltpu.VMEM((rest * each, count), jnp.bfloat16),
        ],
        compiler_params=pltpu.CompilerParams(vmem_limit_bytes=48 * 1024 * 1024),
        name="bands",
    )(me, lags, observers.reshape(1, -1), arrived, weights)


def swap(value, ranks, sides, rank_mask, side_mask):
    pairs = [
        (r * sides + s, (r ^ rank_mask) * sides + (s ^ side_mask)) for r in range(ranks) for s in range(sides)
    ]
    return lax.ppermute(value, AXES, pairs)


def local(surface_raw, area_normals, kernel_weights, block_map, band_observers, band_lags):
    ranks = lax.axis_size("cfd")
    sides = lax.axis_size("ac")
    me = jnp.stack([lax.axis_index("cfd"), lax.axis_index("ac")]).astype(jnp.int32)
    order = block_map[0, 0]
    count = lax.iota(jnp.int32, ranks)
    block_to = jnp.sum(jnp.where(order[None, :] == count[:, None], count[None, :], 0), axis=1)
    sent = outgoing(surface_raw, area_normals, block_to)
    arrived = lax.all_to_all(sent, "cfd", split_axis=0, concat_axis=0, tiled=True)
    keep, send = bands(me, band_lags, band_observers, arrived, kernel_weights, ranks, sides)
    mid, parts, rest, each, piece = keep.shape
    if parts != sides:
        which = jnp.bitwise_xor(lax.iota(jnp.int32, sides), me[1])

        def by_side(value):
            value = value.reshape(mid, rest, each, sides, piece // sides)
            value = jnp.take(value, which, axis=3)
            return jnp.transpose(value, (0, 3, 1, 2, 4))

        keep, send = by_side(keep), by_side(send)
    got = swap(send, ranks, sides, 1, 0)
    low_sides = min(2, sides)
    high_sides = sides // low_sides
    shape = (mid, high_sides, low_sides) + keep.shape[2:]
    keep, got = keep.reshape(shape), got.reshape(shape)

    def first(x, y):
        return keep[x, :, y].astype(jnp.float32) + got[x, :, y].astype(jnp.float32)

    total = first(0, 0)
    for x, y in [(1, 1), (1, 0), (0, 1)]:
        if x < mid and y < low_sides:
            total = total + swap(first(x, y).astype(jnp.bfloat16), ranks, sides, 2 * x, y).astype(jnp.float32)
    result = total[:, 0]
    for z in range(rest - 1, 0, -1):
        result = result + swap(total[:, z].astype(jnp.bfloat16), ranks, sides, 4 * z, 0).astype(jnp.float32)
    out = result[0]
    for y in range(high_sides - 1, 0, -1):
        out = out + swap(result[y].astype(jnp.bfloat16), ranks, sides, 0, 2 * y).astype(jnp.float32)
    return out


def solution(mesh):
    placed = (
        P(None, ("cfd", "ac"), None),
        P(None, ("cfd", "ac")),
        P(None, None, None, ("cfd", "ac")),
        P("ac", "cfd", None),
        P(),
        P(),
    )
    return jax.shard_map(
        local, mesh=mesh, in_specs=placed, out_specs=P("cfd", "ac"), check_vma=False
    )
```

```python
import functools

import jax
import jax.numpy as jnp
from jax import lax
from jax.experimental import pallas as pl
from jax.experimental.pallas import tpu as pltpu
from jax.sharding import PartitionSpec as P

LANES = 128
AXES = ("cfd", "ac")
SMEM = pl.BlockSpec(memory_space=pltpu.SMEM)
VMEM = pl.BlockSpec(memory_space=pltpu.VMEM)


def pressure_kernel(high, me_ref, order_ref, surface_ref, *out_refs):
    for z in range(high):
        for q in range(4):
            out_refs[z][q] = surface_ref[0, order_ref[jnp.bitwise_xor(me_ref[0], 4 * z + q)]]


def pressure_out(me, order, surface, high):
    comps, blocks, rows, steps = surface.shape
    shape = jax.ShapeDtypeStruct((4, rows, steps), jnp.bfloat16)
    return pl.pallas_call(
        functools.partial(pressure_kernel, high),
        grid=(1,),
        out_shape=(shape,) * high,
        in_specs=[SMEM, SMEM, pl.BlockSpec((1, blocks, rows, steps), lambda i: (0, 0, 0, 0))],
        out_specs=(pl.BlockSpec((4, rows, steps), lambda i: (0, 0, 0)),) * high,
        compiler_params=pltpu.CompilerParams(vmem_limit_bytes=8 * 1024 * 1024),
        name="pressure_out",
    )(me, order, surface)


def thickness_kernel(high, me_ref, order_ref, surface_ref, normals_ref, *refs):
    out_refs, columns_ref = refs[:4], refs[4]
    rows = surface_ref.shape[2]
    normals = normals_ref[...].astype(jnp.float32)
    faces = normals.shape[1]
    square = jnp.concatenate([normals, jnp.zeros((faces - normals.shape[0], faces), jnp.float32)], axis=0)
    columns_ref[...] = jnp.transpose(square).reshape(columns_ref.shape)
    for q in range(4):
        for z in range(high):
            block = order_ref[jnp.bitwise_xor(me_ref[0], 4 * z + q)]
            normal = columns_ref[block]
            along = surface_ref[2, block].astype(jnp.float32) * normal[:, 0:1]
            along = along + surface_ref[3, block].astype(jnp.float32) * normal[:, 1:2]
            along = along + surface_ref[4, block].astype(jnp.float32) * normal[:, 2:3]
            out_refs[q][z] = (surface_ref[1, block].astype(jnp.float32) * along).astype(jnp.bfloat16)


def thickness_out(me, order, surface, normals, high):
    comps, blocks, rows, steps = surface.shape
    shape = jax.ShapeDtypeStruct((high, rows, steps), jnp.bfloat16)
    return pl.pallas_call(
        functools.partial(thickness_kernel, high),
        out_shape=(shape,) * 4,
        in_specs=[SMEM, SMEM, VMEM, VMEM],
        out_specs=(VMEM,) * 4,
        scratch_shapes=[pltpu.VMEM((blocks, rows, blocks * rows), jnp.float32)],
        compiler_params=pltpu.CompilerParams(vmem_limit_bytes=8 * 1024 * 1024),
        name="thickness_out",
    )(me, order, surface, normals)


def prepare_kernel(ranks, layout, me_ref, observers_ref, weights_ref, select_ref, joined_ref):
    taps, terms, observers, faces = weights_ref.shape
    for k in range(taps):
        for c in range(terms):
            at = (k * terms + c) * faces
            joined_ref[:, at : at + faces] = weights_ref[k, c]
    each = observers // ranks
    ids = observers_ref[...]
    local_row = lax.broadcasted_iota(jnp.int32, (each, observers), 0)
    for position, member in enumerate(layout):
        base = jnp.bitwise_xor(me_ref[0], member) * each
        chosen = jnp.where(local_row == ids - base, 1.0, 0.0).astype(jnp.bfloat16)
        select_ref[position * each : (position + 1) * each, :] = chosen


def prepare(me, observers, weights, ranks, layout):
    taps, terms, count, faces = weights.shape
    return pl.pallas_call(
        functools.partial(prepare_kernel, ranks, layout),
        out_shape=(
            jax.ShapeDtypeStruct((count, count), jnp.bfloat16),
            jax.ShapeDtypeStruct((count, taps * terms * faces), jnp.bfloat16),
        ),
        in_specs=[SMEM, VMEM, VMEM],
        out_specs=(VMEM, VMEM),
        cost_estimate=pl.CostEstimate(flops=4 * 10**9, bytes_accessed=weights.size * 4, transcendentals=0),
        compiler_params=pltpu.CompilerParams(vmem_limit_bytes=24 * 1024 * 1024),
        name="prepare",
    )(me, observers.reshape(1, -1), weights)


def order_rows(me_ref, select_ref, first_row, banded_ref, out_refs):
    rows = out_refs[0].shape[1]
    parts = out_refs[0].shape[0]
    piece = out_refs[0].shape[2]
    for c, out_ref in enumerate(out_refs):
        at = first_row + c * rows
        chosen = select_ref[at : at + rows, :]
        for y in range(parts):
            if parts == 1:
                data = banded_ref[...]
            else:
                column = pl.multiple_of(jnp.bitwise_xor(me_ref[1], y) * piece, piece)
                data = banded_ref[:, pl.ds(column, piece)]
            out_ref[y] = jnp.dot(chosen, data, preferred_element_type=jnp.float32).astype(jnp.bfloat16)


def place_blocks(me_ref, series_ref, blocks):
    for distance, value in blocks:
        rows = value.shape[0]
        source = jnp.bitwise_xor(me_ref[0], distance)
        value = value.astype(jnp.float32)
        if rows % 8 == 0:
            series_ref[pl.ds(pl.multiple_of(source * rows, 8), rows), :] = value
        else:
            for r in range(rows):
                series_ref[pl.ds(source * rows + r, 1), :] = value[r : r + 1]


def bands_kernel(taps, high, me_ref, lags_ref, joined_ref, select_ref, *refs):
    pressure_refs, refs = refs[: high + 3], refs[high + 3 :]
    thick_refs, refs = refs[: high + 3], refs[high + 3 :]
    banded_ref, keep_ref, send_ref, stacked_ref, series_ref = refs
    faces, steps = series_ref.shape
    terms = joined_ref.shape[1] // faces // taps
    span = stacked_ref.shape[1]
    observers, out_len = banded_ref.shape
    bands = lags_ref.shape[0]
    width = observers // bands
    wide = out_len + LANES
    pairs = [(z, q) for z in range(high) for q in range(4)]
    thick = [(4 * z + q, thick_refs[3 + z][q] if z else thick_refs[q][0]) for z, q in pairs]
    pressure = [(4 * z + q, pressure_refs[high - 1 + q][z] if q else pressure_refs[z][0]) for z, q in pairs]
    pad = jnp.zeros((faces, span - steps), jnp.bfloat16)
    for kind, blocks in enumerate((thick, pressure)):
        place_blocks(me_ref, series_ref, blocks)
        series = series_ref[...]
        earlier = pltpu.roll(series, 1, 1)
        first = lax.broadcasted_iota(jnp.int32, series.shape, 1) == 0
        rate = jnp.where(first, 0.0, series - earlier)
        made = [(kind, rate)] if kind == 0 else [(1, rate), (2, series)]
        for term, value in made:
            for tap in range(taps):
                moved = pltpu.roll(value, tap, 1) if tap else value
                at = (tap * terms + term) * faces
                stacked_ref[at : at + faces, 0:steps] = moved.astype(jnp.bfloat16)
                stacked_ref[at : at + faces, steps:span] = pad

    def one_band(b, carry):
        start = out_len - lags_ref[b]
        column = pl.multiple_of((start // LANES) * LANES, LANES)
        rest = start % LANES
        at = pl.ds(pl.multiple_of(b * width, width), width)
        full = jnp.dot(joined_ref[at, :], stacked_ref[:, pl.ds(column, wide)], preferred_element_type=jnp.float32)
        turned = pltpu.roll(full, (wide - rest) % wide, 1)
        banded_ref[at, :] = turned[:, :out_len].astype(jnp.bfloat16)
        return carry

    lax.fori_loop(0, bands, one_band, 0, unroll=4)
    order_rows(me_ref, select_ref, 0, banded_ref, (keep_ref, send_ref))


def bands(me, lags, pressure, thick, joined, select, taps, parts, rows):
    count = joined.shape[0]
    steps = thick[0].shape[2]
    out_len = steps // 2
    high = len(thick) - 3
    faces = 4 * high * thick[0].shape[1]
    shape = jax.ShapeDtypeStruct((parts, rows, out_len // parts), jnp.bfloat16)
    return pl.pallas_call(
        functools.partial(bands_kernel, taps, high),
        out_shape=(jax.ShapeDtypeStruct((count, out_len), jnp.bfloat16), shape, shape),
        in_specs=[SMEM, SMEM, VMEM, VMEM] + [VMEM] * (2 * (high + 3)),
        out_specs=(VMEM, VMEM, VMEM),
        scratch_shapes=[
            pltpu.VMEM((joined.shape[1], steps + LANES), jnp.bfloat16),
            pltpu.VMEM((faces, steps), jnp.float32),
        ],
        cost_estimate=pl.CostEstimate(flops=4 * 10**9, bytes_accessed=10**7, transcendentals=0),
        compiler_params=pltpu.CompilerParams(vmem_limit_bytes=24 * 1024 * 1024),
        name="bands",
    )(me, lags, joined, select, *pressure, *thick)


def order_kernel(first_row, me_ref, banded_ref, select_ref, keep_ref, send_ref):
    order_rows(me_ref, select_ref, first_row, banded_ref, (keep_ref, send_ref))


def order_more(me, banded, select, first_row, parts, rows):
    shape = jax.ShapeDtypeStruct((parts, rows, banded.shape[1] // parts), jnp.bfloat16)
    return pl.pallas_call(
        functools.partial(order_kernel, first_row),
        out_shape=(shape, shape),
        in_specs=[SMEM, VMEM, VMEM],
        out_specs=(VMEM, VMEM),
        cost_estimate=pl.CostEstimate(flops=2 * 10**9, bytes_accessed=10**7, transcendentals=0),
        compiler_params=pltpu.CompilerParams(vmem_limit_bytes=24 * 1024 * 1024),
        name="order",
    )(me, banded, select)


def swap(value, ranks, sides, rank_mask, side_mask):
    pairs = [
        (r * sides + s, (r ^ rank_mask) * sides + (s ^ side_mask)) for r in range(ranks) for s in range(sides)
    ]
    return lax.ppermute(value, AXES, pairs)


def local(surface_raw, area_normals, kernel_weights, block_map, band_observers, band_lags):
    ranks = lax.axis_size("cfd")
    sides = lax.axis_size("ac")
    me = jnp.stack([lax.axis_index("cfd"), lax.axis_index("ac")]).astype(jnp.int32)
    order = block_map[0, 0]
    high = ranks // 4
    comps, faces, steps = surface_raw.shape
    surface = surface_raw.reshape(comps, ranks, faces // ranks, steps)
    pressure = list(pressure_out(me, order, surface, high))
    thick = list(thickness_out(me, order, surface, area_normals, high))
    for z in range(high - 1, 0, -1):
        pressure[z] = swap(pressure[z], ranks, sides, 4 * z, 0)
    for q in range(3, 0, -1):
        thick[q] = swap(thick[q], ranks, sides, q, 0)
    for q in range(1, 4):
        pressure.append(swap(jnp.stack([pressure[z][q] for z in range(high)]), ranks, sides, q, 0))
    onward = [swap(jnp.stack([thick[q][z] for q in range(4)]), ranks, sides, 4 * z, 0) for z in range(high - 1, 0, -1)]
    thick.extend(reversed(onward))
    taps, _, count_rows, _ = kernel_weights.shape
    out_len = surface_raw.shape[2] // 2
    each = count_rows // ranks
    rest = ranks // 4
    near = rest // 2
    chunks = (range(near, rest), range(near))
    layout = [(z * 2 + x) * 2 + c for zs in chunks for c in range(2) for x in range(2) for z in zs]
    parts = sides if out_len // sides % LANES == 0 else 1
    rows = near * 2 * each
    select, joined = prepare(me, band_observers, kernel_weights, ranks, layout)
    banded, *far = bands(me, band_lags, pressure, thick, joined, select, taps, parts, rows)
    which = jnp.bitwise_xor(lax.iota(jnp.int32, sides), me[1])

    def by_side(value):
        if parts != sides:
            value = value.reshape(rows, sides, out_len // sides)
            value = jnp.transpose(jnp.take(value, which, axis=1), (1, 0, 2))
        return value.reshape(sides // 2, 2, 2, near, each, out_len // sides)

    def exchange(keep, send):
        got = by_side(swap(send, ranks, sides, 1, 0))
        keep = by_side(keep)

        def first(x, y):
            return keep[:, y, x].astype(jnp.float32) + got[:, y, x].astype(jnp.float32)

        total = first(0, 0)
        for x, y in [(1, 1), (1, 0), (0, 1)]:
            total = total + swap(first(x, y).astype(jnp.bfloat16), ranks, sides, 2 * x, y).astype(jnp.float32)
        return total

    def over_z(result, total, zs):
        for z in reversed(zs):
            moved = total[:, z - zs[0]]
            if z:
                moved = swap(moved.astype(jnp.bfloat16), ranks, sides, 4 * z, 0).astype(jnp.float32)
            result = moved if result is None else result + moved
        return result

    result = over_z(None, exchange(*far), chunks[0])
    result = over_z(result, exchange(*order_more(me, banded, select, 2 * rows, parts, rows)), chunks[1])
    out = result[0]
    for y in range(sides // 2 - 1, 0, -1):
        out = out + swap(result[y].astype(jnp.bfloat16), ranks, sides, 0, 2 * y).astype(jnp.float32)
    return out


def solution(mesh):
    placed = (
        P(None, ("cfd", "ac"), None),
        P(None, ("cfd", "ac")),
        P(None, None, None, ("cfd", "ac")),
        P("ac", "cfd", None),
        P(),
        P(),
    )
    return jax.shard_map(
        local, mesh=mesh, in_specs=placed, out_specs=P("cfd", "ac"), check_vma=False
    )
```

```python
import functools

import jax
import jax.numpy as jnp
from jax import lax
from jax.experimental import pallas as pl
from jax.experimental.pallas import tpu as pltpu
from jax.sharding import PartitionSpec as P

LANES = 128
AXES = ("cfd", "ac")
MIDDLE = ((1, 1), (1, 0), (0, 1))
MIB = 1024 * 1024
SMEM = pl.BlockSpec(memory_space=pltpu.SMEM)
VMEM = pl.BlockSpec(memory_space=pltpu.VMEM)
HBM = pl.BlockSpec(memory_space=pltpu.HBM)


def params(mib):
    return pltpu.CompilerParams(vmem_limit_bytes=mib * MIB)


def distance_from_me(distance):
    return jnp.bitwise_xor(lax.axis_index("cfd"), distance)


def outgoing_kernel(direct, high, order_hbm, surface_hbm, normals_hbm, *refs):
    direct_refs, refs = refs[:direct], refs[direct:]
    early_refs, (order_ref, surface_ref, normals_ref, columns_ref, sems) = refs[:4], refs[4:]
    loads = [
        pltpu.make_async_copy(order_hbm, order_ref, sems.at[0]),
        pltpu.make_async_copy(normals_hbm, normals_ref, sems.at[1]),
        pltpu.make_async_copy(surface_hbm, surface_ref, sems.at[2]),
    ]
    for load in loads:
        load.start()
    loads[1].wait()
    normals = normals_ref[...].astype(jnp.float32)
    faces = normals.shape[1]
    square = jnp.concatenate([normals, jnp.zeros((faces - normals.shape[0], faces), jnp.float32)], axis=0)
    columns_ref[...] = jnp.transpose(square).reshape(columns_ref.shape)
    loads[0].wait()
    loads[2].wait()
    for z in range(high):
        for q in range(4):
            block = order_ref[0, distance_from_me(4 * z + q)]
            normal = columns_ref[block]
            along = surface_ref[2, block].astype(jnp.float32) * normal[:, 0:1]
            along = along + surface_ref[3, block].astype(jnp.float32) * normal[:, 1:2]
            along = along + surface_ref[4, block].astype(jnp.float32) * normal[:, 2:3]
            out = direct_refs[z].at[q] if z < direct else early_refs[q].at[z - direct]
            out[0] = (surface_ref[1, block].astype(jnp.float32) * along).astype(jnp.bfloat16)
            out[1] = surface_ref[0, block]


def outgoing(order, surface, normals, direct, high):
    comps, blocks, rows, steps = surface.shape
    shape = lambda lead: jax.ShapeDtypeStruct((lead, 2, rows, steps), jnp.bfloat16)
    return pl.pallas_call(
        functools.partial(outgoing_kernel, direct, high),
        out_shape=(shape(4),) * direct + (shape(high - direct),) * 4,
        in_specs=[HBM, HBM, HBM],
        out_specs=(VMEM,) * (direct + 4),
        scratch_shapes=[
            pltpu.SMEM(order.shape, jnp.int32),
            pltpu.VMEM(surface.shape, jnp.bfloat16),
            pltpu.VMEM(normals.shape, jnp.bfloat16),
            pltpu.VMEM((blocks, rows, blocks * rows), jnp.float32),
            pltpu.SemaphoreType.DMA((3,)),
        ],
        compiler_params=params(8),
        name="outgoing",
    )(*(pltpu.with_memory_space_constraint(x, pltpu.HBM) for x in (order, surface, normals)))


def prepare_kernel(ranks, layout, observers_ref, weights_ref, select_ref, joined_ref):
    taps, terms, observers, faces = weights_ref.shape
    for k in range(taps):
        for c in range(terms):
            at = (k * terms + c) * faces
            joined_ref[:, at : at + faces] = weights_ref[k, c]
    each = observers // ranks
    ids = observers_ref[...]
    local_row = lax.broadcasted_iota(jnp.int32, (each, observers), 0)
    for position, member in enumerate(layout):
        base = distance_from_me(member) * each
        chosen = jnp.where(local_row == ids - base, 1.0, 0.0).astype(jnp.bfloat16)
        select_ref[position * each : (position + 1) * each, :] = chosen


def prepare(observers, weights, ranks, layout):
    taps, terms, count, faces = weights.shape
    return pl.pallas_call(
        functools.partial(prepare_kernel, ranks, layout),
        out_shape=(
            jax.ShapeDtypeStruct((count, count), jnp.bfloat16),
            jax.ShapeDtypeStruct((count, taps * terms * faces), jnp.bfloat16),
        ),
        in_specs=[VMEM, VMEM],
        out_specs=(VMEM, VMEM),
        cost_estimate=pl.CostEstimate(flops=2 * 10**9, bytes_accessed=10**7, transcendentals=0),
        compiler_params=params(24),
        name="prepare",
    )(observers.reshape(1, -1), weights)


def place_block(series_ref, distance, block):
    rows = block.shape[1]
    source = distance_from_me(distance)
    for kind in range(2):
        value = block[kind].astype(jnp.float32)
        if rows % 8 == 0:
            series_ref[kind, pl.ds(pl.multiple_of(source * rows, 8), rows), :] = value
        else:
            for r in range(rows):
                series_ref[kind, pl.ds(source * rows + r, 1), :] = value[r : r + 1]


def order_rows(select_ref, first_row, banded_ref, out_ref):
    parts, rows, piece = out_ref.shape
    chosen = select_ref[first_row : first_row + rows, :]
    for y in range(parts):
        if parts == 1:
            data = banded_ref[...]
        else:
            column = pl.multiple_of(jnp.bitwise_xor(lax.axis_index("ac"), y) * piece, piece)
            data = banded_ref[:, pl.ds(column, piece)]
        out_ref[y] = jnp.dot(chosen, data, preferred_element_type=jnp.float32).astype(jnp.bfloat16)


def bands_kernel(taps, direct, high, first_row, lags_ref, joined_ref, select_ref, *refs):
    near_refs, refs = refs[:direct], refs[direct:]
    post_refs, refs = refs[:3], refs[3:]
    late_refs, refs = refs[: high - direct], refs[high - direct :]
    banded_ref, send_ref, stacked_ref, series_ref = refs
    _, faces, steps = series_ref.shape
    terms = joined_ref.shape[1] // faces // taps
    span = stacked_ref.shape[1]
    observers, out_len = banded_ref.shape
    bands = lags_ref.shape[0]
    width = observers // bands
    wide = out_len + LANES
    for z in range(high):
        for q in range(4):
            if z >= direct:
                block = late_refs[z - direct][q]
            else:
                block = post_refs[q - 1][z] if q else near_refs[z][0]
            place_block(series_ref, 4 * z + q, block)
    stacked_ref[:, steps:span] = jnp.zeros((stacked_ref.shape[0], span - steps), jnp.bfloat16)
    first = lax.broadcasted_iota(jnp.int32, (faces, steps), 1) == 0
    for kind in range(2):
        series = series_ref[kind]
        rate = jnp.where(first, 0.0, series - pltpu.roll(series, 1, 1))
        for term, value in [(0, rate)] if kind == 0 else [(1, rate), (2, series)]:
            for tap in range(taps):
                moved = pltpu.roll(value, tap, 1) if tap else value
                at = (tap * terms + term) * faces
                stacked_ref[at : at + faces, 0:steps] = moved.astype(jnp.bfloat16)

    def one_band(b, carry):
        start = out_len - lags_ref[b]
        column = pl.multiple_of((start // LANES) * LANES, LANES)
        rest = start % LANES
        at = pl.ds(pl.multiple_of(b * width, width), width)
        full = jnp.dot(joined_ref[at, :], stacked_ref[:, pl.ds(column, wide)], preferred_element_type=jnp.float32)
        turned = pltpu.roll(full, (wide - rest) % wide, 1)
        banded_ref[at, :] = turned[:, :out_len].astype(jnp.bfloat16)
        return carry

    lax.fori_loop(0, bands, one_band, 0, unroll=4)
    order_rows(select_ref, first_row, banded_ref, send_ref)


def bands(lags, near, post, late, joined, select, first_row, taps, shape):
    count = joined.shape[0]
    steps = near[0].shape[-1]
    out_len = steps // 2
    direct, high = len(near), len(near) + len(late)
    faces = 4 * high * near[0].shape[2]
    return pl.pallas_call(
        functools.partial(bands_kernel, taps, direct, high, first_row),
        out_shape=(jax.ShapeDtypeStruct((count, out_len), jnp.bfloat16), shape),
        in_specs=[SMEM] + [VMEM] * (high + 5),
        out_specs=(VMEM, VMEM),
        scratch_shapes=[
            pltpu.VMEM((joined.shape[1], steps + LANES), jnp.bfloat16),
            pltpu.VMEM((2, faces, steps), jnp.float32),
        ],
        cost_estimate=pl.CostEstimate(flops=4 * 10**9, bytes_accessed=10**7, transcendentals=0),
        compiler_params=params(24),
        name="bands",
    )(lags, joined, select, *near, *post, *late)


def order_kernel(first_row, banded_ref, select_ref, *refs):
    out_ref = refs[-1]
    order_rows(select_ref, first_row, banded_ref, out_ref)


def order_more(banded, select, first_row, shape, after=()):
    return pl.pallas_call(
        functools.partial(order_kernel, first_row),
        out_shape=shape,
        in_specs=[VMEM] * (2 + len(after)),
        out_specs=VMEM,
        cost_estimate=pl.CostEstimate(flops=10**9, bytes_accessed=5 * 10**6, transcendentals=0),
        compiler_params=params(16),
        name="order",
    )(banded, select, *after)


def swap(value, ranks, sides, rank_mask, side_mask=0):
    pairs = [
        (r * sides + s, (r ^ rank_mask) * sides + (s ^ side_mask)) for r in range(ranks) for s in range(sides)
    ]
    return lax.ppermute(value, AXES, pairs)


def local(surface_raw, area_normals, kernel_weights, block_map, band_observers, band_lags):
    ranks = lax.axis_size("cfd")
    sides = lax.axis_size("ac")
    high = ranks // 4
    direct = high - max(1, high // 4)
    comps, faces, steps = surface_raw.shape
    surface = surface_raw.reshape(comps, ranks, faces // ranks, steps)
    made = outgoing(block_map.reshape(1, ranks), surface, area_normals, direct, high)
    near, early = list(made[:direct]), list(made[direct:])
    for z in range(direct - 1, 0, -1):
        near[z] = swap(near[z], ranks, sides, 4 * z)
    for q in range(3, 0, -1):
        early[q] = swap(early[q], ranks, sides, q)
    late = [
        swap(jnp.stack([early[q][z - direct] for q in range(4)]), ranks, sides, 4 * z) for z in range(direct, high)
    ]
    post = [swap(jnp.stack([near[z][q] for z in range(direct)]), ranks, sides, q) for q in range(1, 4)]

    taps, _, count, _ = kernel_weights.shape
    out_len = steps // 2
    each = count // ranks
    half = high // 2
    chunks = (range(half, high), range(half))
    layout = [(z * 2 + x) * 2 + c for zs in chunks for c in (1, 0) for x in range(2) for z in zs]
    parts = sides if out_len // sides % LANES == 0 else 1
    rows = half * 2 * each
    shape = jax.ShapeDtypeStruct((parts, rows, out_len // parts), jnp.bfloat16)
    select, joined = prepare(band_observers, kernel_weights, ranks, layout)
    banded, far_send = bands(band_lags, near, post, late, joined, select, 0, taps, shape)
    which = jnp.bitwise_xor(lax.iota(jnp.int32, sides), lax.axis_index("ac"))

    def by_side(value):
        if parts != sides:
            value = value.reshape(rows, sides, out_len // sides)
            value = jnp.transpose(jnp.take(value, which, axis=1), (1, 0, 2))
        return value.reshape(sides // 2, 2, 2, half, each, out_len // sides)

    def over_core(send, keep_from):
        got = by_side(swap(send, ranks, sides, 1))
        keep = by_side(order_more(banded, select, keep_from, shape))
        total = lambda x, y: keep[:, y, x].astype(jnp.float32) + got[:, y, x].astype(jnp.float32)
        return total(0, 0), [total(x, y).astype(jnp.bfloat16) for x, y in MIDDLE]

    def over_middle(total, sends):
        for (x, y), send in zip(MIDDLE, sends):
            total = total + swap(send, ranks, sides, 2 * x, y).astype(jnp.float32)
        return total

    def over_z(result, total, zs):
        for z in reversed(zs):
            moved = total[:, z - zs[0]]
            if z:
                moved = swap(moved.astype(jnp.bfloat16), ranks, sides, 4 * z).astype(jnp.float32)
            result = moved if result is None else result + moved
        return result

    far_total, far_sends = over_core(far_send, rows)
    near_send = order_more(banded, select, 2 * rows, shape, far_sends)
    near_total, near_sends = over_core(near_send, 3 * rows)
    result = over_z(None, over_middle(far_total, far_sends), chunks[0])
    result = over_z(result, over_middle(near_total, near_sends), chunks[1])
    out = result[0]
    for y in range(sides // 2 - 1, 0, -1):
        out = out + swap(result[y].astype(jnp.bfloat16), ranks, sides, 0, 2 * y).astype(jnp.float32)
    return out


def solution(mesh):
    placed = (
        P(None, ("cfd", "ac"), None),
        P(None, ("cfd", "ac")),
        P(None, None, None, ("cfd", "ac")),
        P("ac", "cfd", None),
        P(),
        P(),
    )
    return jax.shard_map(
        local, mesh=mesh, in_specs=placed, out_specs=P("cfd", "ac"), check_vma=False
    )
```

```python
import functools

import jax
import jax.numpy as jnp
from jax import lax
from jax.experimental import pallas as pl
from jax.experimental.pallas import tpu as pltpu
from jax.sharding import PartitionSpec as P


LANES = 128
AXES = ("cfd", "ac")
MIDDLE = ((1, 1), (1, 0), (0, 1))
MIB = 1024 * 1024
SMEM = pl.BlockSpec(memory_space=pltpu.SMEM)
VMEM = pl.BlockSpec(memory_space=pltpu.VMEM)
HBM = pl.BlockSpec(memory_space=pltpu.HBM)


def params(mib):
    return pltpu.CompilerParams(vmem_limit_bytes=mib * MIB)


def distance_from_me(distance):
    return jnp.bitwise_xor(lax.axis_index("cfd"), distance)


def outgoing_kernel(direct, high, order_hbm, surface_hbm, normals_hbm, *refs):
    direct_refs, refs = refs[:direct], refs[direct:]
    early_refs, (order_ref, surface_ref, normals_ref, columns_ref, sems) = refs[:4], refs[4:]
    loads = [
        pltpu.make_async_copy(order_hbm, order_ref, sems.at[0]),
        pltpu.make_async_copy(normals_hbm, normals_ref, sems.at[1]),
        pltpu.make_async_copy(surface_hbm, surface_ref, sems.at[2]),
    ]
    for load in loads:
        load.start()
    loads[1].wait()
    normals = normals_ref[...].astype(jnp.float32)
    faces = normals.shape[1]
    square = jnp.concatenate([normals, jnp.zeros((faces - normals.shape[0], faces), jnp.float32)], axis=0)
    columns_ref[...] = jnp.transpose(square).reshape(columns_ref.shape)
    loads[0].wait()
    loads[2].wait()
    for z in range(high):
        for q in range(4):
            block = order_ref[0, distance_from_me(4 * z + q)]
            normal = columns_ref[block]
            along = surface_ref[2, block].astype(jnp.float32) * normal[:, 0:1]
            along = along + surface_ref[3, block].astype(jnp.float32) * normal[:, 1:2]
            along = along + surface_ref[4, block].astype(jnp.float32) * normal[:, 2:3]
            out = direct_refs[z].at[q] if z < direct else early_refs[q].at[z - direct]
            out[0] = (surface_ref[1, block].astype(jnp.float32) * along).astype(jnp.bfloat16)
            out[1] = surface_ref[0, block]


def outgoing(order, surface, normals, direct, high):
    _, blocks, rows, steps = surface.shape
    shape = lambda lead: jax.ShapeDtypeStruct((lead, 2, rows, steps), jnp.bfloat16)
    return pl.pallas_call(
        functools.partial(outgoing_kernel, direct, high),
        out_shape=(shape(4),) * direct + (shape(high - direct),) * 4,
        in_specs=[HBM, HBM, HBM],
        out_specs=(VMEM,) * (direct + 4),
        scratch_shapes=[
            pltpu.SMEM(order.shape, jnp.int32),
            pltpu.VMEM(surface.shape, jnp.bfloat16),
            pltpu.VMEM(normals.shape, jnp.bfloat16),
            pltpu.VMEM((blocks, rows, blocks * rows), jnp.float32),
            pltpu.SemaphoreType.DMA((3,)),
        ],
        compiler_params=params(8),
        name="outgoing",
    )(*(pltpu.with_memory_space_constraint(x, pltpu.HBM) for x in (order, surface, normals)))


def prepare_kernel(ranks, layout, observers_hbm, weights_hbm, select_ref, joined_ref, ids_ref, sems):
    taps, terms, observers, faces = weights_hbm.shape
    loads = [pltpu.make_async_copy(observers_hbm, ids_ref, sems.at[0])]
    for k in range(taps):
        for c in range(terms):
            at = (k * terms + c) * faces
            loads.append(
                pltpu.make_async_copy(
                    weights_hbm.at[k, c], joined_ref.at[:, pl.ds(at, faces)], sems.at[1 + k * terms + c]
                )
            )
    for load in loads:
        load.start()
    loads[0].wait()
    each = observers // ranks
    ids = ids_ref[...]
    local_row = lax.broadcasted_iota(jnp.int32, (each, observers), 0)
    for position, member in enumerate(layout):
        base = distance_from_me(member) * each
        chosen = jnp.where(local_row == ids - base, 1.0, 0.0).astype(jnp.bfloat16)
        select_ref[position * each : (position + 1) * each, :] = chosen
    for load in loads[1:]:
        load.wait()


def prepare(observers, weights, ranks, layout):
    taps, terms, count, faces = weights.shape
    operands = (observers.reshape(1, -1), weights)
    return pl.pallas_call(
        functools.partial(prepare_kernel, ranks, layout),
        out_shape=(
            jax.ShapeDtypeStruct((count, count), jnp.bfloat16),
            jax.ShapeDtypeStruct((count, taps * terms * faces), jnp.bfloat16),
        ),
        in_specs=[HBM, HBM],
        out_specs=(VMEM, VMEM),
        scratch_shapes=[
            pltpu.VMEM((1, count), jnp.int32),
            pltpu.SemaphoreType.DMA((1 + taps * terms,)),
        ],
        cost_estimate=pl.CostEstimate(flops=2 * 10**9, bytes_accessed=10**7, transcendentals=0),
        compiler_params=params(24),
        name="prepare",
    )(*(pltpu.with_memory_space_constraint(x, pltpu.HBM) for x in operands))


def place_block(series_ref, distance, block):
    rows = block.shape[1]
    source = distance_from_me(distance)
    for kind in range(2):
        value = block[kind].astype(jnp.float32)
        if rows % 8 == 0:
            series_ref[kind, pl.ds(pl.multiple_of(source * rows, 8), rows), :] = value
        else:
            for r in range(rows):
                series_ref[kind, pl.ds(source * rows + r, 1), :] = value[r : r + 1]


def order_rows(select_ref, first_row, banded_ref, out_ref):
    parts, rows, piece = out_ref.shape
    chosen = select_ref[first_row : first_row + rows, :]
    for y in range(parts):
        if parts == 1:
            data = banded_ref[...]
        else:
            column = pl.multiple_of(jnp.bitwise_xor(lax.axis_index("ac"), y) * piece, piece)
            data = banded_ref[:, pl.ds(column, piece)]
        out_ref[y] = jnp.dot(chosen, data, preferred_element_type=jnp.float32).astype(jnp.bfloat16)


def bands_kernel(taps, direct, high, first_row, lags_ref, joined_ref, select_ref, *refs):
    near_refs, refs = refs[:direct], refs[direct:]
    post_refs, refs = refs[:3], refs[3:]
    late_refs, refs = refs[: high - direct], refs[high - direct :]
    banded_ref, send_ref, stacked_ref, series_ref = refs
    _, faces, steps = series_ref.shape
    terms = joined_ref.shape[1] // faces // taps
    span = stacked_ref.shape[1]
    observers, out_len = banded_ref.shape
    bands = lags_ref.shape[0]
    width = observers // bands
    wide = out_len + LANES
    for z in range(high):
        for q in range(4):
            if z >= direct:
                block = late_refs[z - direct][q]
            else:
                block = post_refs[q - 1][z] if q else near_refs[z][0]
            place_block(series_ref, 4 * z + q, block)
    stacked_ref[:, steps:span] = jnp.zeros((stacked_ref.shape[0], span - steps), jnp.bfloat16)
    first = lax.broadcasted_iota(jnp.int32, (faces, steps), 1) == 0
    for kind in range(2):
        series = series_ref[kind]
        rate = jnp.where(first, 0.0, series - pltpu.roll(series, 1, 1))
        for term, value in [(0, rate)] if kind == 0 else [(1, rate), (2, series)]:
            for tap in range(taps):
                moved = pltpu.roll(value, tap, 1) if tap else value
                at = (tap * terms + term) * faces
                stacked_ref[at : at + faces, 0:steps] = moved.astype(jnp.bfloat16)

    def one_band(b, carry):
        start = out_len - lags_ref[b]
        column = pl.multiple_of((start // LANES) * LANES, LANES)
        rest = start % LANES
        at = pl.ds(pl.multiple_of(b * width, width), width)
        full = jnp.dot(joined_ref[at, :], stacked_ref[:, pl.ds(column, wide)], preferred_element_type=jnp.float32)
        turned = pltpu.roll(full, (wide - rest) % wide, 1)
        banded_ref[at, :] = turned[:, :out_len].astype(jnp.bfloat16)
        return carry

    lax.fori_loop(0, bands, one_band, 0, unroll=4)
    order_rows(select_ref, first_row, banded_ref, send_ref)


def bands(lags, near, post, late, joined, select, first_row, taps, shape):
    count = joined.shape[0]
    steps = near[0].shape[-1]
    out_len = steps // 2
    direct, high = len(near), len(near) + len(late)
    faces = 4 * high * near[0].shape[2]
    return pl.pallas_call(
        functools.partial(bands_kernel, taps, direct, high, first_row),
        out_shape=(jax.ShapeDtypeStruct((count, out_len), jnp.bfloat16), shape),
        in_specs=[SMEM] + [VMEM] * (high + 5),
        out_specs=(VMEM, VMEM),
        scratch_shapes=[
            pltpu.VMEM((joined.shape[1], steps + LANES), jnp.bfloat16),
            pltpu.VMEM((2, faces, steps), jnp.float32),
        ],
        cost_estimate=pl.CostEstimate(flops=4 * 10**9, bytes_accessed=10**7, transcendentals=0),
        compiler_params=params(24),
        name="bands",
    )(lags, joined, select, *near, *post, *late)


def order_kernel(first_row, banded_ref, select_ref, *refs):
    out_ref = refs[-1]
    order_rows(select_ref, first_row, banded_ref, out_ref)


def order_more(banded, select, first_row, shape, after=()):
    return pl.pallas_call(
        functools.partial(order_kernel, first_row),
        out_shape=shape,
        in_specs=[VMEM] * (2 + len(after)),
        out_specs=VMEM,
        cost_estimate=pl.CostEstimate(flops=10**9, bytes_accessed=5 * 10**6, transcendentals=0),
        compiler_params=params(16),
        name="order",
    )(banded, select, *after)


def total_kernel(keep_ref, got_ref, *refs):
    moved_refs, out_refs = refs[: len(MIDDLE)], refs[-keep_ref.shape[3] :]
    for z, out_ref in enumerate(out_refs):
        total = keep_ref[:, 0, 0, z].astype(jnp.float32) + got_ref[:, 0, 0, z].astype(jnp.float32)
        for moved_ref in moved_refs:
            total = total + moved_ref[:, z].astype(jnp.float32)
        out_ref[...] = total.astype(out_ref.dtype)


def total_far(keep, got, moved, after):
    shape = jax.ShapeDtypeStruct(keep.shape[:1] + keep.shape[4:], jnp.bfloat16)
    half = keep.shape[3]
    return pl.pallas_call(
        total_kernel,
        out_shape=(shape,) * half,
        in_specs=[VMEM] * (2 + len(moved) + len(after)),
        out_specs=(VMEM,) * half,
        compiler_params=params(16),
        name="total_far",
    )(keep, got, *moved, *after)


def swap(value, ranks, sides, rank_mask, side_mask=0):
    pairs = [
        (r * sides + s, (r ^ rank_mask) * sides + (s ^ side_mask)) for r in range(ranks) for s in range(sides)
    ]
    return lax.ppermute(value, AXES, pairs)


def local(surface_raw, area_normals, kernel_weights, block_map, band_observers, band_lags):
    ranks = lax.axis_size("cfd")
    sides = lax.axis_size("ac")
    high = ranks // 4
    direct = high - max(1, high // 4)
    comps, faces, steps = surface_raw.shape
    surface = surface_raw.reshape(comps, ranks, faces // ranks, steps)
    made = outgoing(block_map.reshape(1, ranks), surface, area_normals, direct, high)
    near, early = list(made[:direct]), list(made[direct:])
    for z in range(1, direct):
        near[z] = swap(near[z], ranks, sides, 4 * z)
    for q in range(3, 0, -1):
        early[q] = swap(early[q], ranks, sides, q)
    late = [swap(jnp.stack([early[q][z - direct] for q in range(4)]), ranks, sides, 4 * z) for z in range(direct, high)]
    post = [swap(jnp.stack([near[z][q] for z in range(direct)]), ranks, sides, q) for q in range(1, 4)]

    taps, _, count, _ = kernel_weights.shape
    out_len = steps // 2
    each = count // ranks
    half = high // 2
    chunks = (range(half, high), range(half))
    layout = [(z * 2 + x) * 2 + c for zs in chunks for c in (1, 0) for x in range(2) for z in zs]
    parts = sides if out_len // sides % LANES == 0 else 1
    rows = half * 2 * each
    shape = jax.ShapeDtypeStruct((parts, rows, out_len // parts), jnp.bfloat16)
    select, joined = prepare(band_observers, kernel_weights, ranks, layout)
    banded, far_send = bands(band_lags, near, post, late, joined, select, 0, taps, shape)
    which = jnp.bitwise_xor(lax.iota(jnp.int32, sides), lax.axis_index("ac"))

    def by_side(value):
        if parts != sides:
            value = value.reshape(rows, sides, out_len // sides)
            value = jnp.transpose(jnp.take(value, which, axis=1), (1, 0, 2))
        return value.reshape(sides // 2, 2, 2, half, each, out_len // sides)

    def over_core(send, keep_from):
        got = by_side(swap(send, ranks, sides, 1))
        keep = by_side(order_more(banded, select, keep_from, shape))
        total = lambda x, y: keep[:, y, x].astype(jnp.float32) + got[:, y, x].astype(jnp.float32)
        return keep, got, total(0, 0), [total(x, y).astype(jnp.bfloat16) for x, y in MIDDLE]

    def over_middle(sends):
        return [swap(send, ranks, sides, 2 * x, y) for (x, y), send in zip(MIDDLE, sends)]

    keep, got, _, far_sends = over_core(far_send, rows)
    near_send = order_more(banded, select, 2 * rows, shape, far_sends)
    _, _, total, near_sends = over_core(near_send, 3 * rows)
    moved = over_middle(far_sends)
    far = total_far(keep, got, moved, near_sends)
    for moved in over_middle(near_sends):
        total = total + moved.astype(jnp.float32)
    result = total[:, 0]
    for z in range(high - 1, 0, -1):
        send = far[z - half] if z >= half else total[:, z].astype(jnp.bfloat16)
        result = result + swap(send, ranks, sides, 4 * z).astype(jnp.float32)
    out = result[0]
    for y in range(sides // 2 - 1, 0, -1):
        out = out + swap(result[y].astype(jnp.bfloat16), ranks, sides, 0, 2 * y).astype(jnp.float32)
    return out


def solution(mesh):
    placed = (
        P(None, ("cfd", "ac"), None),
        P(None, ("cfd", "ac")),
        P(None, None, None, ("cfd", "ac")),
        P("ac", "cfd", None),
        P(),
        P(),
    )

    return jax.shard_map(local, mesh=mesh, in_specs=placed, out_specs=P("cfd", "ac"), check_vma=False)
```

```python
import functools

import jax
import jax.numpy as jnp
from jax import lax
from jax.experimental import pallas as pl
from jax.experimental.pallas import tpu as pltpu
from jax.sharding import PartitionSpec as P


LANES = 128
AXES = ("cfd", "ac")
MIDDLE = ((1, 1), (1, 0), (0, 1))
MIB = 1024 * 1024
SMEM = pl.BlockSpec(memory_space=pltpu.SMEM)
VMEM = pl.BlockSpec(memory_space=pltpu.VMEM)
HBM = pl.BlockSpec(memory_space=pltpu.HBM)


def params(mib):
    return pltpu.CompilerParams(vmem_limit_bytes=mib * MIB)


def distance_from_me(distance):
    return jnp.bitwise_xor(lax.axis_index("cfd"), distance)


def outgoing_kernel(direct, high, order_hbm, surface_hbm, normals_hbm, *refs):
    direct_refs, refs = refs[:direct], refs[direct:]
    early_refs, (order_ref, surface_ref, normals_ref, columns_ref, sems) = refs[:4], refs[4:]
    loads = [
        pltpu.make_async_copy(order_hbm, order_ref, sems.at[0]),
        pltpu.make_async_copy(normals_hbm, normals_ref, sems.at[1]),
        pltpu.make_async_copy(surface_hbm, surface_ref, sems.at[2]),
    ]
    for load in loads:
        load.start()
    loads[1].wait()
    normals = normals_ref[...].astype(jnp.float32)
    faces = normals.shape[1]
    square = jnp.concatenate([normals, jnp.zeros((faces - normals.shape[0], faces), jnp.float32)], axis=0)
    columns_ref[...] = jnp.transpose(square).reshape(columns_ref.shape)
    loads[0].wait()
    loads[2].wait()
    for z in range(high):
        for q in range(4):
            block = order_ref[0, distance_from_me(4 * z + q)]
            normal = columns_ref[block]
            along = surface_ref[2, block].astype(jnp.float32) * normal[:, 0:1]
            along = along + surface_ref[3, block].astype(jnp.float32) * normal[:, 1:2]
            along = along + surface_ref[4, block].astype(jnp.float32) * normal[:, 2:3]
            out = direct_refs[z].at[q] if z < direct else early_refs[q].at[z - direct]
            out[0] = (surface_ref[1, block].astype(jnp.float32) * along).astype(jnp.bfloat16)
            out[1] = surface_ref[0, block]


def outgoing(order, surface, normals, direct, high):
    _, blocks, rows, steps = surface.shape
    shape = lambda lead: jax.ShapeDtypeStruct((lead, 2, rows, steps), jnp.bfloat16)
    return pl.pallas_call(
        functools.partial(outgoing_kernel, direct, high),
        out_shape=(shape(4),) * direct + (shape(high - direct),) * 4,
        in_specs=[HBM, HBM, HBM],
        out_specs=(VMEM,) * (direct + 4),
        scratch_shapes=[
            pltpu.SMEM(order.shape, jnp.int32),
            pltpu.VMEM(surface.shape, jnp.bfloat16),
            pltpu.VMEM(normals.shape, jnp.bfloat16),
            pltpu.VMEM((blocks, rows, blocks * rows), jnp.float32),
            pltpu.SemaphoreType.DMA((3,)),
        ],
        compiler_params=params(8),
        name="outgoing",
    )(*(pltpu.with_memory_space_constraint(x, pltpu.HBM) for x in (order, surface, normals)))


def prepare_kernel(ranks, layout, observers_hbm, weights_hbm, select_ref, joined_ref, ids_ref, sems):
    taps, terms, observers, faces = weights_hbm.shape
    loads = [pltpu.make_async_copy(observers_hbm, ids_ref, sems.at[0])]
    for k in range(taps):
        for c in range(terms):
            at = (k * terms + c) * faces
            loads.append(
                pltpu.make_async_copy(
                    weights_hbm.at[k, c], joined_ref.at[:, pl.ds(at, faces)], sems.at[1 + k * terms + c]
                )
            )
    for load in loads:
        load.start()
    loads[0].wait()
    each = observers // ranks
    ids = ids_ref[...]
    local_row = lax.broadcasted_iota(jnp.int32, (each, observers), 0)
    for position, member in enumerate(layout):
        base = distance_from_me(member) * each
        chosen = jnp.where(local_row == ids - base, 1.0, 0.0).astype(jnp.bfloat16)
        select_ref[position * each : (position + 1) * each, :] = chosen
    for load in loads[1:]:
        load.wait()


def prepare(observers, weights, ranks, layout):
    taps, terms, count, faces = weights.shape
    operands = (observers.reshape(1, -1), weights)
    return pl.pallas_call(
        functools.partial(prepare_kernel, ranks, layout),
        out_shape=(
            jax.ShapeDtypeStruct((count, count), jnp.bfloat16),
            jax.ShapeDtypeStruct((count, taps * terms * faces), jnp.bfloat16),
        ),
        in_specs=[HBM, HBM],
        out_specs=(VMEM, VMEM),
        scratch_shapes=[
            pltpu.VMEM((1, count), jnp.int32),
            pltpu.SemaphoreType.DMA((1 + taps * terms,)),
        ],
        cost_estimate=pl.CostEstimate(flops=2 * 10**9, bytes_accessed=10**7, transcendentals=0),
        compiler_params=params(24),
        name="prepare",
    )(*(pltpu.with_memory_space_constraint(x, pltpu.HBM) for x in operands))


def place_block(series_ref, distance, block):
    rows = block.shape[1]
    source = distance_from_me(distance)
    for kind in range(2):
        value = block[kind].astype(jnp.float32)
        if rows % 8 == 0:
            series_ref[kind, pl.ds(pl.multiple_of(source * rows, 8), rows), :] = value
        else:
            for r in range(rows):
                series_ref[kind, pl.ds(source * rows + r, 1), :] = value[r : r + 1]


def order_rows(select_ref, first_row, banded_ref, out_ref):
    parts, rows, piece = out_ref.shape
    chosen = select_ref[first_row : first_row + rows, :]
    for y in range(parts):
        if parts == 1:
            data = banded_ref[...]
        else:
            column = pl.multiple_of(jnp.bitwise_xor(lax.axis_index("ac"), y) * piece, piece)
            data = banded_ref[:, pl.ds(column, piece)]
        out_ref[y] = jnp.dot(chosen, data, preferred_element_type=jnp.float32).astype(jnp.bfloat16)


def bands_kernel(taps, direct, high, first_row, lags_ref, joined_ref, select_ref, *refs):
    near_refs, refs = refs[:direct], refs[direct:]
    post_refs, refs = refs[:3], refs[3:]
    late_refs, refs = refs[: high - direct], refs[high - direct :]
    banded_ref, send_ref, stacked_ref, series_ref = refs
    _, faces, steps = series_ref.shape
    terms = joined_ref.shape[1] // faces // taps
    span = stacked_ref.shape[1]
    observers, out_len = banded_ref.shape
    bands = lags_ref.shape[0]
    width = observers // bands
    wide = out_len + LANES
    for z in range(high):
        for q in range(4):
            if z >= direct:
                block = late_refs[z - direct][q]
            else:
                block = post_refs[q - 1][z] if q else near_refs[z][0]
            place_block(series_ref, 4 * z + q, block)
    stacked_ref[:, steps:span] = jnp.zeros((stacked_ref.shape[0], span - steps), jnp.bfloat16)
    first = lax.broadcasted_iota(jnp.int32, (faces, steps), 1) == 0
    for kind in range(2):
        series = series_ref[kind]
        rate = jnp.where(first, 0.0, series - pltpu.roll(series, 1, 1))
        for term, value in [(0, rate)] if kind == 0 else [(1, rate), (2, series)]:
            for tap in range(taps):
                moved = pltpu.roll(value, tap, 1) if tap else value
                at = (tap * terms + term) * faces
                stacked_ref[at : at + faces, 0:steps] = moved.astype(jnp.bfloat16)

    def one_band(b, carry):
        start = out_len - lags_ref[b]
        column = pl.multiple_of((start // LANES) * LANES, LANES)
        rest = start % LANES
        at = pl.ds(pl.multiple_of(b * width, width), width)
        full = jnp.dot(joined_ref[at, :], stacked_ref[:, pl.ds(column, wide)], preferred_element_type=jnp.float32)
        turned = pltpu.roll(full, (wide - rest) % wide, 1)
        banded_ref[at, :] = turned[:, :out_len].astype(jnp.bfloat16)
        return carry

    lax.fori_loop(0, bands, one_band, 0, unroll=True)
    order_rows(select_ref, first_row, banded_ref, send_ref)


def bands(lags, near, post, late, joined, select, first_row, taps, shape):
    count = joined.shape[0]
    steps = near[0].shape[-1]
    out_len = steps // 2
    direct, high = len(near), len(near) + len(late)
    faces = 4 * high * near[0].shape[2]
    return pl.pallas_call(
        functools.partial(bands_kernel, taps, direct, high, first_row),
        out_shape=(jax.ShapeDtypeStruct((count, out_len), jnp.bfloat16), shape),
        in_specs=[SMEM] + [VMEM] * (high + 5),
        out_specs=(VMEM, VMEM),
        scratch_shapes=[
            pltpu.VMEM((joined.shape[1], steps + LANES), jnp.bfloat16),
            pltpu.VMEM((2, faces, steps), jnp.float32),
        ],
        cost_estimate=pl.CostEstimate(flops=4 * 10**9, bytes_accessed=10**7, transcendentals=0),
        compiler_params=params(24),
        name="bands",
    )(lags, joined, select, *near, *post, *late)


def order_kernel(first_row, banded_ref, select_ref, *refs):
    out_ref = refs[-1]
    order_rows(select_ref, first_row, banded_ref, out_ref)


def order_more(banded, select, first_row, shape, after=()):
    return pl.pallas_call(
        functools.partial(order_kernel, first_row),
        out_shape=shape,
        in_specs=[VMEM] * (2 + len(after)),
        out_specs=VMEM,
        cost_estimate=pl.CostEstimate(flops=10**9, bytes_accessed=5 * 10**6, transcendentals=0),
        compiler_params=params(16),
        name="order",
    )(banded, select, *after)


def total_kernel(keep_ref, got_ref, *refs):
    moved_refs, out_refs = refs[: len(MIDDLE)], refs[-keep_ref.shape[3] :]
    for z, out_ref in enumerate(out_refs):
        total = keep_ref[:, 0, 0, z].astype(jnp.float32) + got_ref[:, 0, 0, z].astype(jnp.float32)
        for moved_ref in moved_refs:
            total = total + moved_ref[:, z].astype(jnp.float32)
        out_ref[...] = total.astype(out_ref.dtype)


def total_far(keep, got, moved, after):
    shape = jax.ShapeDtypeStruct(keep.shape[:1] + keep.shape[4:], jnp.bfloat16)
    half = keep.shape[3]
    return pl.pallas_call(
        total_kernel,
        out_shape=(shape,) * half,
        in_specs=[VMEM] * (2 + len(moved) + len(after)),
        out_specs=(VMEM,) * half,
        compiler_params=params(16),
        name="total_far",
    )(keep, got, *moved, *after)


def swap(value, ranks, sides, rank_mask, side_mask=0):
    pairs = [
        (r * sides + s, (r ^ rank_mask) * sides + (s ^ side_mask)) for r in range(ranks) for s in range(sides)
    ]
    return lax.ppermute(value, AXES, pairs)


def local(surface_raw, area_normals, kernel_weights, block_map, band_observers, band_lags):
    ranks = lax.axis_size("cfd")
    sides = lax.axis_size("ac")
    high = ranks // 4
    direct = high - max(1, high // 4)
    comps, faces, steps = surface_raw.shape
    surface = surface_raw.reshape(comps, ranks, faces // ranks, steps)
    made = outgoing(block_map.reshape(1, ranks), surface, area_normals, direct, high)
    near, early = list(made[:direct]), list(made[direct:])
    for z in range(1, direct):
        near[z] = swap(near[z], ranks, sides, 4 * z)
    for q in range(3, 0, -1):
        early[q] = swap(early[q], ranks, sides, q)
    late = [swap(jnp.stack([early[q][z - direct] for q in range(4)]), ranks, sides, 4 * z) for z in range(direct, high)]
    post = [swap(jnp.stack([near[z][q] for z in range(direct)]), ranks, sides, q) for q in range(1, 4)]

    taps, _, count, _ = kernel_weights.shape
    out_len = steps // 2
    each = count // ranks
    chunks = (range(1, high), range(1))
    layout = [(z * 2 + x) * 2 + c for zs in chunks for c in (1, 0) for x in range(2) for z in zs]
    parts = sides if out_len // sides % LANES == 0 else 1
    far_rows, near_rows = [len(zs) * 2 * each for zs in chunks]
    far_shape, near_shape = [
        jax.ShapeDtypeStruct((parts, rows, out_len // parts), jnp.bfloat16) for rows in (far_rows, near_rows)
    ]
    select, joined = prepare(band_observers, kernel_weights, ranks, layout)
    banded, far_send = bands(band_lags, near, post, late, joined, select, 0, taps, far_shape)
    which = jnp.bitwise_xor(lax.iota(jnp.int32, sides), lax.axis_index("ac"))

    def by_side(value):
        if parts != sides:
            value = value.reshape(-1, sides, out_len // sides)
            value = jnp.transpose(jnp.take(value, which, axis=1), (1, 0, 2))
        return value.reshape(sides // 2, 2, 2, -1, each, out_len // sides)

    def over_core(send, keep_from, shape):
        got = by_side(swap(send, ranks, sides, 1))
        keep = by_side(order_more(banded, select, keep_from, shape))
        total = lambda x, y: keep[:, y, x].astype(jnp.float32) + got[:, y, x].astype(jnp.float32)
        return keep, got, total(0, 0), [total(x, y).astype(jnp.bfloat16) for x, y in MIDDLE]

    def over_middle(sends):
        return [swap(send, ranks, sides, 2 * x, y) for (x, y), send in zip(MIDDLE, sends)]

    keep, got, _, far_sends = over_core(far_send, far_rows, far_shape)
    near_send = order_more(banded, select, 2 * far_rows, near_shape, far_sends)
    _, _, total, near_sends = over_core(near_send, 2 * far_rows + near_rows, near_shape)
    moved = over_middle(far_sends)
    far = total_far(keep, got, moved, near_sends)
    for moved in over_middle(near_sends):
        total = total + moved.astype(jnp.float32)
    result = total[:, 0]
    for z in range(high - 1, 0, -1):
        result = result + swap(far[z - 1], ranks, sides, 4 * z).astype(jnp.float32)
    out = result[0]
    for y in range(sides // 2 - 1, 0, -1):
        out = out + swap(result[y].astype(jnp.bfloat16), ranks, sides, 0, 2 * y).astype(jnp.float32)
    return out


def solution(mesh):
    placed = (
        P(None, ("cfd", "ac"), None),
        P(None, ("cfd", "ac")),
        P(None, None, None, ("cfd", "ac")),
        P("ac", "cfd", None),
        P(),
        P(),
    )

    return jax.shard_map(local, mesh=mesh, in_specs=placed, out_specs=P("cfd", "ac"), check_vma=False)
```

```python
import functools

import jax
import jax.numpy as jnp
from jax import lax
from jax.experimental import pallas as pl
from jax.experimental.pallas import tpu as pltpu
from jax.sharding import PartitionSpec as P


LANES = 128
AXES = ("cfd", "ac")
MIDDLE = ((1, 0), (0, 1), (1, 1))
MIB = 1024 * 1024
SMEM = pl.BlockSpec(memory_space=pltpu.SMEM)
VMEM = pl.BlockSpec(memory_space=pltpu.VMEM)
HBM = pl.BlockSpec(memory_space=pltpu.HBM)


def params(mib):
    return pltpu.CompilerParams(vmem_limit_bytes=mib * MIB)


def distance_from_me(distance):
    return jnp.bitwise_xor(lax.axis_index("cfd"), distance)


def outgoing_kernel(direct, high, order_hbm, surface_hbm, normals_hbm, *refs):
    direct_refs, refs = refs[:direct], refs[direct:]
    early_refs, (order_ref, surface_ref, normals_ref, columns_ref, sems) = refs[:4], refs[4:]
    loads = [
        pltpu.make_async_copy(order_hbm, order_ref, sems.at[0]),
        pltpu.make_async_copy(normals_hbm, normals_ref, sems.at[1]),
        pltpu.make_async_copy(surface_hbm, surface_ref, sems.at[2]),
    ]
    for load in loads:
        load.start()
    loads[1].wait()
    normals = normals_ref[...].astype(jnp.float32)
    faces = normals.shape[1]
    square = jnp.concatenate([normals, jnp.zeros((faces - normals.shape[0], faces), jnp.float32)], axis=0)
    columns_ref[...] = jnp.transpose(square).reshape(columns_ref.shape)
    loads[0].wait()
    loads[2].wait()
    for z in range(high):
        for q in range(4):
            block = order_ref[0, distance_from_me(4 * z + q)]
            normal = columns_ref[block]
            along = surface_ref[2, block].astype(jnp.float32) * normal[:, 0:1]
            along = along + surface_ref[3, block].astype(jnp.float32) * normal[:, 1:2]
            along = along + surface_ref[4, block].astype(jnp.float32) * normal[:, 2:3]
            out = direct_refs[z].at[q] if z < direct else early_refs[q].at[z - direct]
            out[0] = (surface_ref[1, block].astype(jnp.float32) * along).astype(jnp.bfloat16)
            out[1] = surface_ref[0, block]


def outgoing(order, surface, normals, direct, high):
    _, blocks, rows, steps = surface.shape
    shape = lambda lead: jax.ShapeDtypeStruct((lead, 2, rows, steps), jnp.bfloat16)
    return pl.pallas_call(
        functools.partial(outgoing_kernel, direct, high),
        out_shape=(shape(4),) * direct + (shape(high - direct),) * 4,
        in_specs=[HBM, HBM, HBM],
        out_specs=(VMEM,) * (direct + 4),
        scratch_shapes=[
            pltpu.SMEM(order.shape, jnp.int32),
            pltpu.VMEM(surface.shape, jnp.bfloat16),
            pltpu.VMEM(normals.shape, jnp.bfloat16),
            pltpu.VMEM((blocks, rows, blocks * rows), jnp.float32),
            pltpu.SemaphoreType.DMA((3,)),
        ],
        compiler_params=params(8),
        name="outgoing",
    )(*(pltpu.with_memory_space_constraint(x, pltpu.HBM) for x in (order, surface, normals)))


def prepare_kernel(ranks, layout, observers_hbm, weights_hbm, select_ref, joined_ref, ids_ref, sems):
    taps, terms, observers, faces = weights_hbm.shape
    loads = [pltpu.make_async_copy(observers_hbm, ids_ref, sems.at[0])]
    for k in range(taps):
        for c in range(terms):
            at = (k * terms + c) * faces
            loads.append(
                pltpu.make_async_copy(
                    weights_hbm.at[k, c], joined_ref.at[:, pl.ds(at, faces)], sems.at[1 + k * terms + c]
                )
            )
    for load in loads:
        load.start()
    loads[0].wait()
    each = observers // ranks
    ids = ids_ref[...]
    local_row = lax.broadcasted_iota(jnp.int32, (each, observers), 0)
    for position, member in enumerate(layout):
        base = distance_from_me(member) * each
        chosen = jnp.where(local_row == ids - base, 1.0, 0.0).astype(jnp.bfloat16)
        select_ref[position * each : (position + 1) * each, :] = chosen
    for load in loads[1:]:
        load.wait()


def prepare(observers, weights, ranks, layout):
    taps, terms, count, faces = weights.shape
    operands = (observers.reshape(1, -1), weights)
    return pl.pallas_call(
        functools.partial(prepare_kernel, ranks, layout),
        out_shape=(
            jax.ShapeDtypeStruct((count, count), jnp.bfloat16),
            jax.ShapeDtypeStruct((count, taps * terms * faces), jnp.bfloat16),
        ),
        in_specs=[HBM, HBM],
        out_specs=(VMEM, VMEM),
        scratch_shapes=[
            pltpu.VMEM((1, count), jnp.int32),
            pltpu.SemaphoreType.DMA((1 + taps * terms,)),
        ],
        cost_estimate=pl.CostEstimate(flops=2 * 10**9, bytes_accessed=10**7, transcendentals=0),
        compiler_params=params(24),
        name="prepare",
    )(*(pltpu.with_memory_space_constraint(x, pltpu.HBM) for x in operands))


def place_block(series_ref, distance, block):
    rows = block.shape[1]
    source = distance_from_me(distance)
    for kind in range(2):
        value = block[kind].astype(jnp.float32)
        if rows % 8 == 0:
            series_ref[kind, pl.ds(pl.multiple_of(source * rows, 8), rows), :] = value
        else:
            for r in range(rows):
                series_ref[kind, pl.ds(source * rows + r, 1), :] = value[r : r + 1]


def order_rows(select_ref, first_row, banded_ref, out_ref):
    parts, rows, piece = out_ref.shape
    chosen = select_ref[first_row : first_row + rows, :]
    for y in range(parts):
        if parts == 1:
            data = banded_ref[...]
        else:
            column = pl.multiple_of(jnp.bitwise_xor(lax.axis_index("ac"), y) * piece, piece)
            data = banded_ref[:, pl.ds(column, piece)]
        out_ref[y] = jnp.dot(chosen, data, preferred_element_type=jnp.float32).astype(jnp.bfloat16)


def bands_kernel(taps, direct, high, first_row, lags_ref, joined_ref, select_ref, *refs):
    near_refs, refs = refs[:direct], refs[direct:]
    post_refs, refs = refs[:3], refs[3:]
    late_refs, refs = refs[: high - direct], refs[high - direct :]
    banded_ref, send_ref, stacked_ref, series_ref = refs
    _, faces, steps = series_ref.shape
    terms = joined_ref.shape[1] // faces // taps
    span = stacked_ref.shape[1]
    observers, out_len = banded_ref.shape
    bands = lags_ref.shape[0]
    width = observers // bands
    wide = out_len + LANES
    for z in range(high):
        for q in range(4):
            if z >= direct:
                block = late_refs[z - direct][q]
            else:
                block = post_refs[q - 1][z] if q else near_refs[z][0]
            place_block(series_ref, 4 * z + q, block)
    stacked_ref[:, steps:span] = jnp.zeros((stacked_ref.shape[0], span - steps), jnp.bfloat16)
    first = lax.broadcasted_iota(jnp.int32, (faces, steps), 1) == 0
    for kind in range(2):
        series = series_ref[kind]
        rate = jnp.where(first, 0.0, series - pltpu.roll(series, 1, 1))
        for term, value in [(0, rate)] if kind == 0 else [(1, rate), (2, series)]:
            for tap in range(taps):
                moved = pltpu.roll(value, tap, 1) if tap else value
                at = (tap * terms + term) * faces
                stacked_ref[at : at + faces, 0:steps] = moved.astype(jnp.bfloat16)

    def one_band(b, carry):
        start = out_len - lags_ref[b]
        column = pl.multiple_of((start // LANES) * LANES, LANES)
        rest = start % LANES
        at = pl.ds(pl.multiple_of(b * width, width), width)
        full = jnp.dot(joined_ref[at, :], stacked_ref[:, pl.ds(column, wide)], preferred_element_type=jnp.float32)
        turned = pltpu.roll(full, (wide - rest) % wide, 1)
        banded_ref[at, :] = turned[:, :out_len].astype(jnp.bfloat16)
        return carry

    lax.fori_loop(0, bands, one_band, 0, unroll=True)
    order_rows(select_ref, first_row, banded_ref, send_ref)


def bands(lags, near, post, late, joined, select, first_row, taps, shape):
    count = joined.shape[0]
    steps = near[0].shape[-1]
    out_len = steps // 2
    direct, high = len(near), len(near) + len(late)
    faces = 4 * high * near[0].shape[2]
    return pl.pallas_call(
        functools.partial(bands_kernel, taps, direct, high, first_row),
        out_shape=(jax.ShapeDtypeStruct((count, out_len), jnp.bfloat16), shape),
        in_specs=[SMEM] + [VMEM] * (high + 5),
        out_specs=(VMEM, VMEM),
        scratch_shapes=[
            pltpu.VMEM((joined.shape[1], steps + LANES), jnp.bfloat16),
            pltpu.VMEM((2, faces, steps), jnp.float32),
        ],
        cost_estimate=pl.CostEstimate(flops=4 * 10**9, bytes_accessed=10**7, transcendentals=0),
        compiler_params=params(24),
        name="bands",
    )(lags, joined, select, *near, *post, *late)


def order_kernel(first_row, banded_ref, select_ref, *refs):
    out_ref = refs[-1]
    order_rows(select_ref, first_row, banded_ref, out_ref)


def order_more(banded, select, first_row, shape, after=()):
    return pl.pallas_call(
        functools.partial(order_kernel, first_row),
        out_shape=shape,
        in_specs=[VMEM] * (2 + len(after)),
        out_specs=VMEM,
        cost_estimate=pl.CostEstimate(flops=10**9, bytes_accessed=5 * 10**6, transcendentals=0),
        compiler_params=params(16),
        name="order",
    )(banded, select, *after)


def total_kernel(keep_ref, got_ref, *refs):
    moved_refs, out_refs = refs[: len(MIDDLE)], refs[-keep_ref.shape[3] :]
    for z, out_ref in enumerate(out_refs):
        total = keep_ref[:, 0, 0, z].astype(jnp.float32) + got_ref[:, 0, 0, z].astype(jnp.float32)
        for moved_ref in moved_refs:
            total = total + moved_ref[:, z].astype(jnp.float32)
        out_ref[...] = total.astype(out_ref.dtype)


def total_far(keep, got, moved, after):
    shape = jax.ShapeDtypeStruct(keep.shape[:1] + keep.shape[4:], jnp.bfloat16)
    half = keep.shape[3]
    return pl.pallas_call(
        total_kernel,
        out_shape=(shape,) * half,
        in_specs=[VMEM] * (2 + len(moved) + len(after)),
        out_specs=(VMEM,) * half,
        compiler_params=params(16),
        name="total_far",
    )(keep, got, *moved, *after)


def swap(value, ranks, sides, rank_mask, side_mask=0):
    pairs = [
        (r * sides + s, (r ^ rank_mask) * sides + (s ^ side_mask)) for r in range(ranks) for s in range(sides)
    ]
    return lax.ppermute(value, AXES, pairs)


def local(surface_raw, area_normals, kernel_weights, block_map, band_observers, band_lags):
    ranks = lax.axis_size("cfd")
    sides = lax.axis_size("ac")
    high = ranks // 4
    direct = high - max(1, high // 4)
    comps, faces, steps = surface_raw.shape
    surface = surface_raw.reshape(comps, ranks, faces // ranks, steps)
    made = outgoing(block_map.reshape(1, ranks), surface, area_normals, direct, high)
    near, early = list(made[:direct]), list(made[direct:])
    for z in range(1, direct):
        near[z] = swap(near[z], ranks, sides, 4 * z)
    for q in range(3, 0, -1):
        early[q] = swap(early[q], ranks, sides, q)
    late = [swap(jnp.stack([early[q][z - direct] for q in range(4)]), ranks, sides, 4 * z) for z in range(direct, high)]
    post = [swap(jnp.stack([near[z][q] for z in range(direct)]), ranks, sides, q) for q in range(1, 4)]

    taps, _, count, _ = kernel_weights.shape
    out_len = steps // 2
    each = count // ranks
    half = high // 2
    chunks = (range(half, high), range(half))
    layout = [(z * 2 + x) * 2 + c for zs in chunks for c in (1, 0) for x in range(2) for z in zs]
    parts = sides if out_len // sides % LANES == 0 else 1
    far_rows, near_rows = [len(zs) * 2 * each for zs in chunks]
    far_shape, near_shape = [
        jax.ShapeDtypeStruct((parts, rows, out_len // parts), jnp.bfloat16) for rows in (far_rows, near_rows)
    ]
    select, joined = prepare(band_observers, kernel_weights, ranks, layout)
    banded, far_send = bands(band_lags, near, post, late, joined, select, 0, taps, far_shape)
    which = jnp.bitwise_xor(lax.iota(jnp.int32, sides), lax.axis_index("ac"))

    def by_side(value):
        if parts != sides:
            value = value.reshape(-1, sides, out_len // sides)
            value = jnp.transpose(jnp.take(value, which, axis=1), (1, 0, 2))
        return value.reshape(sides // 2, 2, 2, -1, each, out_len // sides)

    def over_core(send, keep_from, shape):
        got = by_side(swap(send, ranks, sides, 1))
        keep = by_side(order_more(banded, select, keep_from, shape))
        total = lambda x, y: keep[:, y, x].astype(jnp.float32) + got[:, y, x].astype(jnp.float32)
        return keep, got, total(0, 0), [total(x, y).astype(jnp.bfloat16) for x, y in MIDDLE]

    def over_middle(sends):
        got = []
        for (x, y), send in zip(MIDDLE, sends):
            got.append(swap(send, ranks, sides, 2 * x, y))
        return got

    keep, got, _, far_sends = over_core(far_send, far_rows, far_shape)
    near_send = order_more(banded, select, 2 * far_rows, near_shape, far_sends)
    _, _, total, near_sends = over_core(near_send, 2 * far_rows + near_rows, near_shape)
    moved = over_middle(far_sends)
    far = total_far(keep, got, moved, near_sends)
    for moved in over_middle(near_sends):
        total = total + moved.astype(jnp.float32)
    result = total[:, 0]
    for z in range(high - 1, 0, -1):
        send = far[z - half] if z >= half else total[:, z].astype(jnp.bfloat16)
        result = result + swap(send, ranks, sides, 4 * z).astype(jnp.float32)
    out = result[0]
    for y in range(sides // 2 - 1, 0, -1):
        out = out + swap(result[y].astype(jnp.bfloat16), ranks, sides, 0, 2 * y).astype(jnp.float32)
    return out


def solution(mesh):
    placed = (
        P(None, ("cfd", "ac"), None),
        P(None, ("cfd", "ac")),
        P(None, None, None, ("cfd", "ac")),
        P("ac", "cfd", None),
        P(),
        P(),
    )

    return jax.shard_map(local, mesh=mesh, in_specs=placed, out_specs=P("cfd", "ac"), check_vma=False)
```

```python
import functools

import jax
import jax.numpy as jnp
from jax import lax
from jax.experimental import pallas as pl
from jax.experimental.pallas import tpu as pltpu
from jax.sharding import PartitionSpec as P


LANES = 128
AXES = ("cfd", "ac")
MIDDLE = ((1, 1), (1, 0), (0, 1))
MIB = 1024 * 1024
SMEM = pl.BlockSpec(memory_space=pltpu.SMEM)
VMEM = pl.BlockSpec(memory_space=pltpu.VMEM)
HBM = pl.BlockSpec(memory_space=pltpu.HBM)


def params(mib):
    return pltpu.CompilerParams(vmem_limit_bytes=mib * MIB)


def distance_from_me(distance):
    return jnp.bitwise_xor(lax.axis_index("cfd"), distance)


def outgoing_kernel(direct, high, order_hbm, surface_hbm, normals_hbm, *refs):
    direct_refs, refs = refs[:direct], refs[direct:]
    early_refs, (order_ref, surface_ref, normals_ref, columns_ref, sems) = refs[:4], refs[4:]
    loads = [
        pltpu.make_async_copy(order_hbm, order_ref, sems.at[0]),
        pltpu.make_async_copy(normals_hbm, normals_ref, sems.at[1]),
        pltpu.make_async_copy(surface_hbm, surface_ref, sems.at[2]),
    ]
    for load in loads:
        load.start()
    loads[1].wait()
    normals = normals_ref[...].astype(jnp.float32)
    faces = normals.shape[1]
    square = jnp.concatenate([normals, jnp.zeros((faces - normals.shape[0], faces), jnp.float32)], axis=0)
    columns_ref[...] = jnp.transpose(square).reshape(columns_ref.shape)
    loads[0].wait()
    loads[2].wait()
    for z in range(high):
        for q in range(4):
            block = order_ref[0, distance_from_me(4 * z + q)]
            normal = columns_ref[block]
            along = surface_ref[2, block].astype(jnp.float32) * normal[:, 0:1]
            along = along + surface_ref[3, block].astype(jnp.float32) * normal[:, 1:2]
            along = along + surface_ref[4, block].astype(jnp.float32) * normal[:, 2:3]
            out = direct_refs[z].at[q] if z < direct else early_refs[q].at[z - direct]
            out[0] = (surface_ref[1, block].astype(jnp.float32) * along).astype(jnp.bfloat16)
            out[1] = surface_ref[0, block]


def outgoing(order, surface, normals, direct, high):
    _, blocks, rows, steps = surface.shape
    shape = lambda lead: jax.ShapeDtypeStruct((lead, 2, rows, steps), jnp.bfloat16)
    return pl.pallas_call(
        functools.partial(outgoing_kernel, direct, high),
        out_shape=(shape(4),) * direct + (shape(high - direct),) * 4,
        in_specs=[HBM, HBM, HBM],
        out_specs=(VMEM,) * (direct + 4),
        scratch_shapes=[
            pltpu.SMEM(order.shape, jnp.int32),
            pltpu.VMEM(surface.shape, jnp.bfloat16),
            pltpu.VMEM(normals.shape, jnp.bfloat16),
            pltpu.VMEM((blocks, rows, blocks * rows), jnp.float32),
            pltpu.SemaphoreType.DMA((3,)),
        ],
        compiler_params=params(8),
        name="outgoing",
    )(*(pltpu.with_memory_space_constraint(x, pltpu.HBM) for x in (order, surface, normals)))


def prepare_kernel(ranks, layout, observers_hbm, weights_hbm, select_ref, joined_ref, ids_ref, sems):
    taps, terms, observers, faces = weights_hbm.shape
    loads = [pltpu.make_async_copy(observers_hbm, ids_ref, sems.at[0])]
    for k in range(taps):
        for c in range(terms):
            at = (k * terms + c) * faces
            loads.append(
                pltpu.make_async_copy(
                    weights_hbm.at[k, c], joined_ref.at[:, pl.ds(at, faces)], sems.at[1 + k * terms + c]
                )
            )
    for load in loads:
        load.start()
    loads[0].wait()
    each = observers // ranks
    ids = ids_ref[...]
    local_row = lax.broadcasted_iota(jnp.int32, (each, observers), 0)
    for position, member in enumerate(layout):
        base = distance_from_me(member) * each
        chosen = jnp.where(local_row == ids - base, 1.0, 0.0).astype(jnp.bfloat16)
        select_ref[position * each : (position + 1) * each, :] = chosen
    for load in loads[1:]:
        load.wait()


def prepare(observers, weights, ranks, layout):
    taps, terms, count, faces = weights.shape
    operands = (observers.reshape(1, -1), weights)
    return pl.pallas_call(
        functools.partial(prepare_kernel, ranks, layout),
        out_shape=(
            jax.ShapeDtypeStruct((count, count), jnp.bfloat16),
            jax.ShapeDtypeStruct((count, taps * terms * faces), jnp.bfloat16),
        ),
        in_specs=[HBM, HBM],
        out_specs=(VMEM, VMEM),
        scratch_shapes=[
            pltpu.VMEM((1, count), jnp.int32),
            pltpu.SemaphoreType.DMA((1 + taps * terms,)),
        ],
        cost_estimate=pl.CostEstimate(flops=2 * 10**9, bytes_accessed=10**7, transcendentals=0),
        compiler_params=params(24),
        name="prepare",
    )(*(pltpu.with_memory_space_constraint(x, pltpu.HBM) for x in operands))


def place_block(series_ref, distance, block):
    rows = block.shape[1]
    source = distance_from_me(distance)
    for kind in range(2):
        value = block[kind].astype(jnp.float32)
        if rows % 8 == 0:
            series_ref[kind, pl.ds(pl.multiple_of(source * rows, 8), rows), :] = value
        else:
            for r in range(rows):
                series_ref[kind, pl.ds(source * rows + r, 1), :] = value[r : r + 1]


def order_rows(select_ref, first_row, banded_ref, out_ref):
    parts, rows, piece = out_ref.shape
    chosen = select_ref[first_row : first_row + rows, :]
    for y in range(parts):
        if parts == 1:
            data = banded_ref[...]
        else:
            column = pl.multiple_of(jnp.bitwise_xor(lax.axis_index("ac"), y) * piece, piece)
            data = banded_ref[:, pl.ds(column, piece)]
        out_ref[y] = jnp.dot(chosen, data, preferred_element_type=jnp.float32).astype(jnp.bfloat16)


def bands_kernel(taps, direct, high, first_row, lags_ref, joined_ref, select_ref, *refs):
    near_refs, refs = refs[:direct], refs[direct:]
    post_refs, refs = refs[:3], refs[3:]
    late_refs, refs = refs[: high - direct], refs[high - direct :]
    banded_ref, send_ref, stacked_ref, series_ref = refs
    _, faces, steps = series_ref.shape
    terms = joined_ref.shape[1] // faces // taps
    span = stacked_ref.shape[1]
    observers, out_len = banded_ref.shape
    bands = lags_ref.shape[0]
    width = observers // bands
    wide = out_len + LANES
    for z in range(high):
        for q in range(4):
            if z >= direct:
                block = late_refs[z - direct][q]
            else:
                block = post_refs[q - 1][z] if q else near_refs[z][0]
            place_block(series_ref, 4 * z + q, block)
    stacked_ref[:, steps:span] = jnp.zeros((stacked_ref.shape[0], span - steps), jnp.bfloat16)
    first = lax.broadcasted_iota(jnp.int32, (faces, steps), 1) == 0
    for kind in range(2):
        series = series_ref[kind]
        rate = jnp.where(first, 0.0, series - pltpu.roll(series, 1, 1))
        for term, value in [(0, rate)] if kind == 0 else [(1, rate), (2, series)]:
            for tap in range(taps):
                moved = pltpu.roll(value, tap, 1) if tap else value
                at = (tap * terms + term) * faces
                stacked_ref[at : at + faces, 0:steps] = moved.astype(jnp.bfloat16)

    def one_band(b, carry):
        start = out_len - lags_ref[b]
        column = pl.multiple_of((start // LANES) * LANES, LANES)
        rest = start % LANES
        at = pl.ds(pl.multiple_of(b * width, width), width)
        full = jnp.dot(joined_ref[at, :], stacked_ref[:, pl.ds(column, wide)], preferred_element_type=jnp.float32)
        turned = pltpu.roll(full, (wide - rest) % wide, 1)
        banded_ref[at, :] = turned[:, :out_len].astype(jnp.bfloat16)
        return carry

    lax.fori_loop(0, bands, one_band, 0, unroll=True)
    order_rows(select_ref, first_row, banded_ref, send_ref)


def bands(lags, near, post, late, joined, select, first_row, taps, shape):
    count = joined.shape[0]
    steps = near[0].shape[-1]
    out_len = steps // 2
    direct, high = len(near), len(near) + len(late)
    faces = 4 * high * near[0].shape[2]
    return pl.pallas_call(
        functools.partial(bands_kernel, taps, direct, high, first_row),
        out_shape=(jax.ShapeDtypeStruct((count, out_len), jnp.bfloat16), shape),
        in_specs=[SMEM] + [VMEM] * (high + 5),
        out_specs=(VMEM, VMEM),
        scratch_shapes=[
            pltpu.VMEM((joined.shape[1], steps + LANES), jnp.bfloat16),
            pltpu.VMEM((2, faces, steps), jnp.float32),
        ],
        cost_estimate=pl.CostEstimate(flops=4 * 10**9, bytes_accessed=10**7, transcendentals=0),
        compiler_params=params(24),
        name="bands",
    )(lags, joined, select, *near, *post, *late)


def order_kernel(first_row, banded_ref, select_ref, *refs):
    out_ref = refs[-1]
    order_rows(select_ref, first_row, banded_ref, out_ref)


def order_more(banded, select, first_row, shape, after=()):
    return pl.pallas_call(
        functools.partial(order_kernel, first_row),
        out_shape=shape,
        in_specs=[VMEM] * (2 + len(after)),
        out_specs=VMEM,
        cost_estimate=pl.CostEstimate(flops=10**9, bytes_accessed=5 * 10**6, transcendentals=0),
        compiler_params=params(16),
        name="order",
    )(banded, select, *after)


def total_kernel(keep_ref, got_ref, *refs):
    moved_refs, out_refs = refs[: len(MIDDLE)], refs[-keep_ref.shape[3] :]
    for z, out_ref in enumerate(out_refs):
        total = keep_ref[:, 0, 0, z].astype(jnp.float32) + got_ref[:, 0, 0, z].astype(jnp.float32)
        for moved_ref in moved_refs:
            total = total + moved_ref[:, z].astype(jnp.float32)
        out_ref[...] = total.astype(out_ref.dtype)


def total_far(keep, got, moved, after):
    shape = jax.ShapeDtypeStruct(keep.shape[:1] + keep.shape[4:], jnp.bfloat16)
    half = keep.shape[3]
    return pl.pallas_call(
        total_kernel,
        out_shape=(shape,) * half,
        in_specs=[VMEM] * (2 + len(moved) + len(after)),
        out_specs=(VMEM,) * half,
        compiler_params=params(16),
        name="total_far",
    )(keep, got, *moved, *after)


def swap(value, ranks, sides, rank_mask, side_mask=0):
    pairs = [
        (r * sides + s, (r ^ rank_mask) * sides + (s ^ side_mask)) for r in range(ranks) for s in range(sides)
    ]
    return lax.ppermute(value, AXES, pairs)


def local(surface_raw, area_normals, kernel_weights, block_map, band_observers, band_lags):
    ranks = lax.axis_size("cfd")
    sides = lax.axis_size("ac")
    high = ranks // 4
    direct = high - max(1, high // 4)
    comps, faces, steps = surface_raw.shape
    surface = surface_raw.reshape(comps, ranks, faces // ranks, steps)
    made = outgoing(block_map.reshape(1, ranks), surface, area_normals, direct, high)
    near, early = list(made[:direct]), list(made[direct:])
    for z in range(1, direct):
        near[z] = swap(near[z], ranks, sides, 4 * z)
    for q in range(3, 0, -1):
        early[q] = swap(early[q], ranks, sides, q)
    late = [swap(jnp.stack([early[q][z - direct] for q in range(4)]), ranks, sides, 4 * z) for z in range(direct, high)]
    post = [swap(jnp.stack([near[z][q] for z in range(direct)]), ranks, sides, q) for q in range(1, 4)]

    taps, _, count, _ = kernel_weights.shape
    out_len = steps // 2
    each = count // ranks
    half = high // 2
    chunks = (range(half, high), range(half))
    layout = [(z * 2 + x) * 2 + c for zs in chunks for c in (1, 0) for x in range(2) for z in zs]
    parts = sides if out_len // sides % LANES == 0 else 1
    far_rows, near_rows = [len(zs) * 2 * each for zs in chunks]
    far_shape, near_shape = [
        jax.ShapeDtypeStruct((parts, rows, out_len // parts), jnp.bfloat16) for rows in (far_rows, near_rows)
    ]
    select, joined = prepare(band_observers, kernel_weights, ranks, layout)
    banded, far_send = bands(band_lags, near, post, late, joined, select, 0, taps, far_shape)
    which = jnp.bitwise_xor(lax.iota(jnp.int32, sides), lax.axis_index("ac"))

    def by_side(value):
        if parts != sides:
            value = value.reshape(-1, sides, out_len // sides)
            value = jnp.transpose(jnp.take(value, which, axis=1), (1, 0, 2))
        return value.reshape(sides // 2, 2, 2, -1, each, out_len // sides)

    def over_core(send, keep_from, shape):
        got = by_side(swap(send, ranks, sides, 1))
        keep = by_side(order_more(banded, select, keep_from, shape))
        total = lambda x, y: keep[:, y, x].astype(jnp.float32) + got[:, y, x].astype(jnp.float32)
        return keep, got, total(0, 0), [total(x, y).astype(jnp.bfloat16) for x, y in MIDDLE]

    def over_middle(sends):
        return [swap(send, ranks, sides, 2 * x, y) for (x, y), send in zip(MIDDLE, sends)]

    keep, got, _, far_sends = over_core(far_send, far_rows, far_shape)
    near_send = order_more(banded, select, 2 * far_rows, near_shape, far_sends)
    _, _, total, near_sends = over_core(near_send, 2 * far_rows + near_rows, near_shape)
    moved = over_middle(far_sends)
    far = total_far(keep, got, moved, near_sends)
    for moved in over_middle(near_sends):
        total = total + moved.astype(jnp.float32)
    result = total[:, 0]
    for z in range(high - 1, 0, -1):
        send = far[z - half] if z >= half else total[:, z].astype(jnp.bfloat16)
        result = result + swap(send, ranks, sides, 4 * z).astype(jnp.float32)
    out = result[0]
    for y in range(sides // 2 - 1, 0, -1):
        out = out + swap(result[y].astype(jnp.bfloat16), ranks, sides, 0, 2 * y).astype(jnp.float32)
    return out


def solution(mesh):
    placed = (
        P(None, ("cfd", "ac"), None),
        P(None, ("cfd", "ac")),
        P(None, None, None, ("cfd", "ac")),
        P("ac", "cfd", None),
        P(),
        P(),
    )

    return jax.shard_map(local, mesh=mesh, in_specs=placed, out_specs=P("cfd", "ac"), check_vma=False)
```
